16 devices in a mesh: dp: 4 (over y, z, core), tp: 4 (over x).
Axes of the slice: x: 4, y: 2, z: 1, core: 2. Of those that a mesh axis runs over, the one named last changes fastest.
The devices are a block of a 4x4x8 slice.
Arguments:
- x: bfloat16 [4096, 4096], P(('dp', 'tp')), parts along dimension 0
- dy: bfloat16 [4096, 4096], P(('dp', 'tp')), parts along dimension 0
- gain: bfloat16 [4096], replicated
- wq: bfloat16 [4096, 4096], P(None, 'tp')
- wk: bfloat16 [4096, 512], P(None, 'tp')
- wv: bfloat16 [4096, 512], P(None, 'tp')
- wo: bfloat16 [4096, 4096], P('tp')
Outputs:
- output 1: bfloat16 [4096, 4096], P(('dp', 'tp')), parts along dimension 0
- output 2: float32 [4, 4096], P('dp'), parts along dimension 0
- output 3: bfloat16 [16384, 4096], P('dp', 'tp'), parts along dimension 0
- output 4: bfloat16 [16384, 512], P('dp', 'tp'), parts along dimension 0
- output 5: bfloat16 [16384, 512], P('dp', 'tp'), parts along dimension 0
- output 6: bfloat16 [16384, 4096], P(('dp', 'tp')), parts along dimension 0
There are 4 independent parts. The reference program is written for one: setup_inputs(seed, part) draws one part's arguments, and reference() takes and returns one part's arrays. A program takes and returns all parts, laid end to end along the dimension named above; an argument that names none is the same for every part.
All inputs are finite; a program needn't handle non-finite values.
Results may differ from the reference program's by a relative error of at most 0.018.
Values are sent between devices in bfloat16 or wider.
A program may use at most 768 MiB of HBM per device.

```python
import jax
import jax.numpy as jnp
from jax import lax

ROWS = 1024
D = 4096
HEADS = 32
KV_HEADS = 4
HEAD = 128
THETA = 10000


def setup_inputs(seed: int = 0, part: int = 0) -> dict:
    kx, ky, kn, kq, kk, kv, ko = jax.random.split(jax.random.key(seed), 7)

    def weights(key, rows, columns):
        return jax.random.normal(key, (rows, columns), jnp.float32) * rows**-0.5

    drawn = {
        "x": jax.random.normal(jax.random.fold_in(kx, part), (ROWS, D), jnp.float32),
        "dy": jax.random.normal(jax.random.fold_in(ky, part), (ROWS, D), jnp.float32) * ROWS**-0.5,
        "gain": 1 + 0.1 * jax.random.normal(kn, (D,), jnp.float32),
        "wq": 2 * weights(kq, D, HEADS * HEAD),
        "wk": 2 * weights(kk, D, KV_HEADS * HEAD),
        "wv": 4 * weights(kv, D, KV_HEADS * HEAD),
        "wo": weights(ko, HEADS * HEAD, D),
    }
    return {k: v.astype(jnp.bfloat16) for k, v in drawn.items()}


def normed(x, gain):
    wide = x.astype(jnp.float32)
    scale = lax.rsqrt(jnp.mean(wide * wide, -1, keepdims=True) + 1e-6)
    return (wide * scale * gain.astype(jnp.float32)).astype(jnp.bfloat16)


def turned(t, place, theta):
    half = t.shape[-1] // 2
    angle = place.astype(jnp.float32)[:, None] * theta ** (-jnp.arange(half, dtype=jnp.float32) / half)
    cos, sin = jnp.cos(angle)[:, None], jnp.sin(angle)[:, None]
    a, b = t[..., :half].astype(jnp.float32), t[..., half:].astype(jnp.float32)
    return jnp.concatenate([a * cos - b * sin, b * cos + a * sin], -1).astype(jnp.bfloat16)


def matmul(a, w):
    return jnp.dot(a, w, preferred_element_type=jnp.float32).astype(jnp.bfloat16)


def einsum(form, a, b):
    return jnp.einsum(form, a.astype(jnp.float32), b.astype(jnp.float32))


def attention(q, k, v):
    scores = einsum("tgsd,ugd->gstu", q, k) * q.shape[-1] ** -0.5
    token = jnp.arange(q.shape[0])
    scores = jnp.where(token[:, None] >= token, scores, -jnp.inf)
    weights = jax.nn.softmax(scores, -1).astype(jnp.bfloat16)
    return einsum("gstu,ugd->tgsd", weights, v).astype(jnp.bfloat16)


def forward(x, gain, wq, wk, wv, wo):
    rows = x.shape[0]
    a, place = normed(x, gain), jnp.arange(rows)
    k = turned(matmul(a, wk).reshape(rows, -1, HEAD), place, THETA)
    q = turned(matmul(a, wq).reshape(rows, -1, HEAD), place, THETA).reshape(rows, k.shape[1], -1, HEAD)
    v = matmul(a, wv).reshape(rows, -1, HEAD)
    seen = attention(q, k, v).reshape(rows, -1)
    return (x.astype(jnp.float32) + jnp.dot(seen, wo, preferred_element_type=jnp.float32)).astype(jnp.bfloat16)


def reference(x, dy, gain, wq, wk, wv, wo):
    _, back = jax.vjp(forward, x, gain.astype(jnp.float32), wq, wk, wv, wo)
    by_x, by_gain, *by_weights = back(dy)
    return (by_x, by_gain[None], *by_weights)
```

```python
import functools

import jax
import jax.numpy as jnp
import numpy as np
from jax import lax
from jax.experimental import pallas as pl
from jax.experimental.pallas import tpu as pltpu
from jax.sharding import PartitionSpec as P

HEAD = 128
THETA = 10000
NEG = -1e30
HIDDEN = 2 * NEG
LOG2E = 1.4426950408889634
VMEM = 67043328
STRIP = 512
TILE = 256
F32, BF16 = jnp.float32, jnp.bfloat16


def _dot(a, b, ca, cb):
    return lax.dot_general(a, b, (((ca,), (cb,)), ((), ())), preferred_element_type=F32)


def _later(bk, cols, bq):
    return lax.rem(lax.broadcasted_iota(jnp.int32, (bk, cols), 1), bq) >= lax.broadcasted_iota(jnp.int32, (bk, cols), 0)


def _kernel(n, x_ref, dy_ref, gain_ref, wq_ref, wk_ref, wv_ref, wo_ref, cos_ref, sin_ref,
            a_out, dy_out, seen_out, dqkv_out, own_out, got_out, sum_out, share_out,
            x_vm, a_vm, w_vm, wo_vm, dy_vm, q_vm, seen_vm, ds_vm, dqkv_vm, k_vm, v_vm, dk_s, dv_s, lse_s, top_s, mix_s, dq_s, delta_s,
            cos_vm, sin_vm, scale_s, in_vm, share_vm, send_sem, recv_sem, load_sem, out_sem):
    rows, deep = x_ref.shape
    half = rows // 2
    width, d = wq_ref.shape[1], k_vm.shape[1]
    g = width // d
    per = STRIP // rows
    strips = g // per
    scale = d**-0.5
    e = scale * LOG2E
    me = lax.axis_index("tp")
    to_right, to_left = lax.rem(me + 1, n), lax.rem(me + n - 1, n)
    low, high = pl.ds(0, half), pl.ds(half, half)

    def start_of(s):
        return pl.multiple_of(lax.rem(me + s, n) * rows, rows)

    def send(src, dst, to, i):
        return pltpu.make_async_remote_copy(src_ref=src, dst_ref=dst, send_sem=send_sem.at[i], recv_sem=recv_sem.at[i],
                                            device_id={"tp": to}, device_id_type=pl.DeviceIdType.MESH)

    def load(src, dst, i):
        return pltpu.make_async_copy(src, dst, load_sem.at[i])

    def put(src, dst, i):
        return pltpu.make_async_copy(src, dst, out_sem.at[i])

    def ring(own, at, i):
        return [send(own.at[low], at.at[n - 1, low], to_right, i), send(own.at[high], at.at[1, high], to_left, i + 1),
                send(own.at[high], at.at[n - 1, high], to_right, i + 2), send(own.at[low], at.at[1, low], to_left, i + 3),
                send(at.at[n - 1, low], at.at[2, low], to_right, i + 4), send(at.at[1, high], at.at[2, high], to_left, i + 5)]

    x_ring, dy_ring = ring(x_ref, x_vm, 0), ring(dy_ref, dy_vm, 6)
    loads = [load(x_ref, x_vm.at[0], 0), load(wq_ref, w_vm.at[:, pl.ds(0, width)], 1), load(wk_ref, w_vm.at[:, pl.ds(width, d)], 2),
             load(wv_ref, w_vm.at[:, pl.ds(width + d, d)], 3), load(cos_ref, cos_vm, 4), load(sin_ref, sin_vm, 5),
             load(dy_ref, dy_vm.at[0], 6), load(wo_ref, wo_vm, 7)]

    barrier = pltpu.get_barrier_semaphore()
    for o in range(1, n):
        pl.semaphore_signal(barrier, inc=1, device_id={"tp": lax.rem(me + o, n)}, device_id_type=pl.DeviceIdType.MESH)
    pl.semaphore_wait(barrier, n - 1)
    for c in x_ring[:4]:
        c.start()
    for c in loads:
        c.start()

    def turn(t, s, sign):
        here = pl.ds(start_of(s), rows)
        return t * cos_vm[here, :] + sign * (pltpu.roll(t, d // 2, 1) * sin_vm[here, :])

    def project(i, _):
        s = i + i // 2 - 2 * (i // 3)

        @pl.when(i == 0)
        def _():
            for c in loads[:6]:
                c.wait()

        @pl.when(i == 1)
        def _():
            for c in x_ring[:2]:
                c.wait_recv()
            for c in x_ring[4:] + dy_ring[:4]:
                c.start()
            for c in x_ring[2:4]:
                c.wait_recv()

        @pl.when(i == 3)
        def _():
            for c in x_ring[4:]:
                c.wait_recv()

        @pl.when(i > 0)
        def _():
            put(a_vm, a_out.at[0], 0).wait()

        def norm(r, _):
            some = pl.ds(pl.multiple_of(r * 16, 16), 16)
            t = x_vm[s, some, :].astype(F32)
            factor = lax.rsqrt(jnp.mean(t * t, -1, keepdims=True) + 1e-6)
            scale_s[s, some, :] = jnp.broadcast_to(factor, (16, 128))
            a_vm[some, :] = (t * factor * gain_ref[...]).astype(BF16)

        lax.fori_loop(0, rows // 16, norm, None)
        put(a_vm, a_out.at[s], 0).start()

        def tile(c, _):
            at = pl.multiple_of(c * TILE, TILE)
            t = _dot(a_vm[...], w_vm[:, pl.ds(at, TILE)], 1, 0).astype(BF16).astype(F32)
            for m in range(TILE // d):
                q_vm[s, :, pl.ds(pl.multiple_of(at + m * d, d), d)] = turn(t[:, m * d : (m + 1) * d], s, 1).astype(BF16)

        lax.fori_loop(0, width // TILE, tile, None)
        t = _dot(a_vm[...], w_vm[:, width:], 1, 0).astype(BF16)
        k_vm[pl.ds(start_of(s), rows), :] = turn(t[:, :d].astype(F32), s, 1).astype(BF16)
        v_vm[pl.ds(start_of(s), rows), :] = t[:, d:]

    lax.fori_loop(0, n, project, None)

    def heads(ref, first):
        return jnp.concatenate([ref[:, h * d : (h + 1) * d] for h in range(first, first + per)], axis=0)

    ones = jnp.ones((8, rows), BF16)

    def forward(s, _):
        top_s[...] = jnp.full_like(top_s, NEG)
        mix_s[...] = jnp.zeros_like(mix_s)

        def block(j, masked):
            here = pl.ds(pl.multiple_of(j * rows, rows), rows)
            keys = k_vm[here, :]
            values = jnp.concatenate([v_vm[here, :].T, ones], axis=0)
            scores = [_dot(keys, heads(q_vm.at[s], c * per), 1, 1) for c in range(strips)]
            weights, keeps = [], []
            for c, t in enumerate(scores):
                if masked:
                    t = jnp.where(_later(rows, STRIP, rows), t, HIDDEN)
                old = top_s[c : c + 1, :]
                top = jnp.maximum(old, t.max(axis=0, keepdims=True))
                top_s[c : c + 1, :] = top
                weights.append(jnp.exp2((t - top) * e).astype(BF16))
                keeps.append(jnp.exp2((old - top) * e))
            for c in range(strips):
                mix_s[c] = mix_s[c] * keeps[c] + _dot(values, weights[c], 1, 0)

        whole = lax.rem(me + s, n)
        lax.fori_loop(0, whole, lambda j, _: block(j, False), None)
        block(whole, True)
        for c in range(strips):
            total = mix_s[c, d : d + 1, :]
            out = (mix_s[c, :d, :] * (1 / total)).T
            lse_s[s, c : c + 1, :] = top_s[c : c + 1, :] * e + jnp.log(total) * LOG2E
            for m in range(per):
                h = c * per + m
                seen_vm[s, :, h * d : (h + 1) * d] = out[m * rows : (m + 1) * rows, :].astype(BF16)

    lax.fori_loop(0, n, forward, None)
    put(seen_vm, seen_out, 1).start()

    dk_s[...] = jnp.zeros_like(dk_s)
    dv_s[...] = jnp.zeros_like(dv_s)

    def backward(i, _):
        s = i + i // 2 - 2 * (i // 3)

        @pl.when(i == 0)
        def _():
            for c in loads[6:]:
                c.wait()
            for c in dy_ring[:2]:
                c.wait_recv()
            for c in dy_ring[4:]:
                c.start()

        @pl.when(i == 1)
        def _():
            for c in dy_ring[2:4]:
                c.wait_recv()

        @pl.when(i == 3)
        def _():
            for c in dy_ring[4:]:
                c.wait_recv()

        put(dy_vm.at[s], dy_out.at[s], 2 + s).start()

        def tile(c, _):
            at = pl.ds(pl.multiple_of(c * TILE, TILE), TILE)
            ds_vm[:, at] = _dot(dy_vm[s], wo_vm[at, :], 1, 1).astype(BF16)

        lax.fori_loop(0, width // TILE, tile, None)
        dq_s[...] = jnp.zeros_like(dq_s)
        for h in range(g):
            at = slice(h * d, (h + 1) * d)
            both = ds_vm[:, at].astype(F32) * seen_vm[s, :, at].astype(F32)
            c, m = divmod(h, per)
            delta_s[c : c + 1, m * rows : (m + 1) * rows] = both.T.sum(axis=0, keepdims=True)

        def block(j, masked):
            here = pl.ds(pl.multiple_of(j * rows, rows), rows)
            keys, values = k_vm[here, :], v_vm[here, :]
            qs = [heads(q_vm.at[s], c * per) for c in range(strips)]
            dos = [heads(ds_vm, c * per) for c in range(strips)]
            scores = [_dot(keys, t, 1, 1) for t in qs]
            dps = [_dot(values, t, 1, 1) for t in dos]
            for c in range(strips):
                p = jnp.exp2(scores[c] * e - lse_s[s, c : c + 1, :])
                if masked:
                    p = jnp.where(_later(rows, STRIP, rows), p, 0.0)
                ds = (p * (dps[c] - delta_s[c : c + 1, :])).astype(BF16)
                dv_s[here, :] += _dot(p.astype(BF16), dos[c], 1, 0)
                dk_s[here, :] += _dot(ds, qs[c], 1, 0)
                dq_s[c] += _dot(keys.T, ds, 1, 0)

        whole = lax.rem(me + s, n)
        lax.fori_loop(0, whole, lambda j, _: block(j, False), None)
        block(whole, True)
        for c in range(strips):
            dq = (dq_s[c] * scale).T
            for m in range(per):
                h = c * per + m
                dqkv_vm[s, :, h * d : (h + 1) * d] = turn(dq[m * rows : (m + 1) * rows, :], s, -1).astype(BF16)

    lax.fori_loop(0, n, backward, None)
    for s in range(n):
        here = pl.ds(start_of(s), rows)
        dqkv_vm[s, :, width : width + d] = turn(dk_s[here, :] * scale, s, -1).astype(BF16)
        dqkv_vm[s, :, width + d :] = dv_s[here, :].astype(BF16)
    put(dqkv_vm, dqkv_out, 6).start()
    for s in range(n):
        put(dy_vm.at[s], dy_out.at[s], 2 + s).wait()
    for c in x_ring + dy_ring:
        c.wait_send()

    share = share_vm.at[me]
    share[...] = jnp.zeros_like(share)
    quarter = deep // 4
    first = []
    for p in range(4):
        at = pl.ds(p * quarter, quarter)
        first += [send(dy_vm.at[2, low, at], in_vm.at[0, :, at], to_right, 12 + 2 * p),
                  send(dy_vm.at[2, high, at], in_vm.at[1, :, at], to_left, 13 + 2 * p)]
    second = [send(dy_vm.at[1, high], got_out.at[high], to_right, 20), send(dy_vm.at[n - 1, low], got_out.at[low], to_left, 21)]
    shares = [send(share, share, lax.rem(me + o, n), 21 + o) for o in range(1, n)]

    def term(i, _):
        s = lax.rem(n + 2 - i, n)

        def tile(c, _):
            at = pl.ds(pl.multiple_of(c * TILE, TILE), TILE)
            t = _dot(dqkv_vm[s], w_vm[at, :], 1, 1).astype(BF16)
            dy_vm[s, :, at] = t
            unit = x_vm[s, :, at].astype(F32) * jnp.concatenate([scale_s[s]] * (TILE // 128), axis=1)
            share[:, at] += (t.astype(F32) * unit).reshape(rows // 8, 8, TILE).sum(0)

            for p in range(4):
                @pl.when((i == 0) & (c == (p + 1) * (quarter // TILE) - 1))
                def _():
                    first[2 * p].start()
                    first[2 * p + 1].start()

        lax.fori_loop(0, deep // TILE, tile, None)

        @pl.when(i == 1)
        def _():
            second[0].start()

        @pl.when(i == 3)
        def _():
            second[1].start()

    lax.fori_loop(0, n, term, None)
    for c in shares:
        c.start()
    put(dy_vm.at[0], own_out, 7).start()
    for c in first:
        c.wait_recv()

    def add(r, _):
        some = pl.ds(pl.multiple_of(r * 16, 16), 16)
        there = pl.ds(pl.multiple_of(half + r * 16, 16), 16)
        in_vm[0, some, :] = (dy_vm[1, some, :].astype(F32) + in_vm[0, some, :].astype(F32)).astype(BF16)
        in_vm[1, some, :] = (dy_vm[n - 1, there, :].astype(F32) + in_vm[1, some, :].astype(F32)).astype(BF16)

    lax.fori_loop(0, half // 16, add, None)
    put(in_vm, sum_out, 8).start()
    for c in shares:
        c.wait_recv()
    put(share_vm, share_out, 9).start()
    for c in second:
        c.wait_recv()
    for c in first + second + shares:
        c.wait_send()
    put(a_vm, a_out.at[0], 0).wait()
    for src, dst, i in ((seen_vm, seen_out, 1), (dqkv_vm, dqkv_out, 6), (dy_vm.at[0], own_out, 7), (in_vm, sum_out, 8), (share_vm, share_out, 9)):
        put(src, dst, i).wait()


def gathered(n, x, dy, gain, wq, wk, wv, wo, cos, sin):
    rows, deep = x.shape
    width, d = wq.shape[1], wk.shape[1]
    g, half = width // d, rows // 2
    strips = g * rows // STRIP
    some = pl.BlockSpec(memory_space=pl.ANY)
    out = jax.ShapeDtypeStruct
    return pl.pallas_call(
        functools.partial(_kernel, n),
        in_specs=[some, some, pl.BlockSpec(memory_space=pltpu.VMEM)] + [some] * 6,
        out_specs=[some] * 8,
        out_shape=[out((n, rows, deep), BF16), out((n, rows, deep), BF16), out((n, rows, width), BF16), out((n, rows, width + 2 * d), BF16),
                   out((rows, deep), BF16), out((rows, deep), BF16), out((2, half, deep), BF16), out((n, 8, deep), F32)],
        scratch_shapes=[
            pltpu.VMEM((n, rows, deep), BF16), pltpu.VMEM((rows, deep), BF16), pltpu.VMEM((deep, width + 2 * d), BF16),
            pltpu.VMEM((width, deep), BF16), pltpu.VMEM((n, rows, deep), BF16), pltpu.VMEM((n, rows, width), BF16),
            pltpu.VMEM((n, rows, width), BF16), pltpu.VMEM((rows, width), BF16), pltpu.VMEM((n, rows, width + 2 * d), BF16),
            pltpu.VMEM((n * rows, d), BF16), pltpu.VMEM((n * rows, d), BF16), pltpu.VMEM((n * rows, d), F32), pltpu.VMEM((n * rows, d), F32),
            pltpu.VMEM((n, strips, STRIP), F32), pltpu.VMEM((strips, STRIP), F32), pltpu.VMEM((strips, d + 8, STRIP), F32),
            pltpu.VMEM((strips, d, STRIP), F32), pltpu.VMEM((strips, STRIP), F32), pltpu.VMEM((n * rows, d), F32), pltpu.VMEM((n * rows, d), F32),
            pltpu.VMEM((n, rows, 128), F32), pltpu.VMEM((2, half, deep), BF16), pltpu.VMEM((n, 8, deep), F32),
            pltpu.SemaphoreType.DMA((25,)), pltpu.SemaphoreType.DMA((25,)), pltpu.SemaphoreType.DMA((8,)), pltpu.SemaphoreType.DMA((10,)),
        ],
        compiler_params=pltpu.CompilerParams(collective_id=0, has_side_effects=True, vmem_limit_bytes=VMEM),
        cost_estimate=pl.CostEstimate(flops=60 * rows * deep * width, transcendentals=0, bytes_accessed=20 * rows * deep),
    )(x, dy, gain, wq, wk, wv, wo, cos, sin)


def solution(mesh):
    n = mesh.shape["tp"]

    def step(x, dy, gain, wq, wk, wv, wo):
        rows, deep = x.shape
        half, width = rows // 2, wq.shape[1]
        gain = gain.astype(F32)[None]

        half_head = HEAD // 2
        rate = np.float32(THETA) ** (-np.arange(half_head, dtype=np.float32) / np.float32(half_head))
        angle = np.arange(n * rows, dtype=np.float32)[:, None] * rate
        cos = jnp.asarray(np.concatenate([np.cos(angle)] * 2, 1))
        sin = jnp.asarray(np.concatenate([-np.sin(angle), np.sin(angle)], 1))

        normal, dy_all, seen, dqkv, own, got, sums, shares = gathered(n, x, dy, gain, wq, wk, wv, wo, cos, sin)
        last_a = lax.ppermute(sums[0], "tp", [(i, (i + 1) % n) for i in range(n)])
        last_b = lax.ppermute(sums[1], "tp", [(i, (i - 1) % n) for i in range(n)])

        normal, dy_all, seen, dqkv = (t.reshape(n * rows, -1) for t in (normal, dy_all, seen, dqkv))
        by_wo = _dot(seen, dy_all, 0, 0).astype(BF16)
        by_wq = _dot(normal, dqkv[:, :width], 0, 0).astype(BF16)
        by_wkv = _dot(normal, dqkv[:, width:], 0, 0).astype(BF16)
        by_wk, by_wv = by_wkv[:, :HEAD], by_wkv[:, HEAD:]
        by_gain = shares.sum((0, 1))[None]

        d_normal = own.astype(F32) + got.astype(F32) + jnp.concatenate([last_a, last_b]).astype(F32)
        wide = x.astype(F32)
        scale = lax.rsqrt(jnp.mean(wide * wide, -1, keepdims=True) + 1e-6)
        unit = wide * scale
        d_unit = d_normal * gain
        by_x = scale * (d_unit - unit * jnp.mean(d_unit * unit, -1, keepdims=True)) + dy.astype(F32)
        return by_x.astype(BF16), by_gain, by_wq, by_wk, by_wv, by_wo

    tokens, columns = P(("dp", "tp"), None), P(None, "tp")
    return jax.shard_map(
        step,
        mesh=mesh,
        in_specs=(tokens, tokens, P(None), columns, columns, columns, P("tp", None)),
        out_specs=(tokens, P("dp", None), P("dp", "tp"), P("dp", "tp"), P("dp", "tp"), P(("dp", "tp"), None)),
        check_vma=False,
    )
```

```python
import functools

import jax
import jax.numpy as jnp
import numpy as np
from jax import lax
from jax.experimental import pallas as pl
from jax.experimental.pallas import tpu as pltpu
from jax.sharding import PartitionSpec as P

HEAD = 128
THETA = 10000
NEG = -1e30
HIDDEN = 2 * NEG
LOG2E = 1.4426950408889634
VMEM = 67043328
STRIP = 512
TILE = 256
F32, BF16 = jnp.float32, jnp.bfloat16


def _dot(a, b, ca, cb):
    return lax.dot_general(a, b, (((ca,), (cb,)), ((), ())), preferred_element_type=F32)


def _later(bk, cols, bq):
    return lax.rem(lax.broadcasted_iota(jnp.int32, (bk, cols), 1), bq) >= lax.broadcasted_iota(jnp.int32, (bk, cols), 0)


def _kernel(n, x_ref, dy_ref, gain_ref, wq_ref, wk_ref, wv_ref, wo_ref, cos_ref, sin_ref,
            a_out, dy_out, seen_out, dqkv_out, own_out, right_b_out, left_a_out, sum_a_out, sum_b_out, share_out,
            x_vm, a_vm, w_vm, wo_vm, dy_vm, q_vm, seen_vm, ds_vm, dqkv_vm, k_vm, v_vm, dk_s, dv_s, lse_s, top_s, mix_s, dq_s, delta_s,
            cos_vm, sin_vm, scale_s, in_vm, share_vm, gain_vm, gain_s, dots_vm, send_sem, recv_sem, load_sem, out_sem):
    rows, deep = x_ref.shape
    half = rows // 2
    width, d = wq_ref.shape[1], k_vm.shape[1]
    g = width // d
    per = STRIP // rows
    strips = g // per
    scale = d**-0.5
    e = scale * LOG2E
    me = lax.axis_index("tp")
    to_right, to_left = lax.rem(me + 1, n), lax.rem(me + n - 1, n)
    low, high = pl.ds(0, half), pl.ds(half, half)

    def start_of(s):
        return pl.multiple_of(lax.rem(me + s, n) * rows, rows)

    def send(src, dst, to, i):
        return pltpu.make_async_remote_copy(src_ref=src, dst_ref=dst, send_sem=send_sem.at[i], recv_sem=recv_sem.at[i],
                                            device_id={"tp": to}, device_id_type=pl.DeviceIdType.MESH)

    def load(src, dst, i):
        return pltpu.make_async_copy(src, dst, load_sem.at[i])

    def put(src, dst, i):
        return pltpu.make_async_copy(src, dst, out_sem.at[i])

    def ring(own, at, i):
        return [send(own.at[low], at.at[n - 1, low], to_right, i), send(own.at[high], at.at[1, high], to_left, i + 1),
                send(own.at[high], at.at[n - 1, high], to_right, i + 2), send(own.at[low], at.at[1, low], to_left, i + 3),
                send(at.at[n - 1, low], at.at[2, low], to_right, i + 4), send(at.at[1, high], at.at[2, high], to_left, i + 5)]

    x_ring, dy_ring = ring(x_ref, x_vm, 0), ring(dy_ref, dy_vm, 6)
    loads = [load(x_ref, x_vm.at[0], 0), load(wq_ref, w_vm.at[:, pl.ds(0, width)], 1), load(wk_ref, w_vm.at[:, pl.ds(width, d)], 2),
             load(wv_ref, w_vm.at[:, pl.ds(width + d, d)], 3), load(cos_ref, cos_vm, 4), load(sin_ref, sin_vm, 5),
             load(dy_ref, dy_vm.at[0], 6), load(wo_ref, wo_vm, 7)]

    barrier = pltpu.get_barrier_semaphore()
    for o in range(1, n):
        pl.semaphore_signal(barrier, inc=1, device_id={"tp": lax.rem(me + o, n)}, device_id_type=pl.DeviceIdType.MESH)
    pl.semaphore_wait(barrier, n - 1)
    for c in x_ring[:4]:
        c.start()
    for c in loads:
        c.start()

    gain_vm[...] = gain_ref[...].astype(F32).reshape(1, deep)

    def turn(t, s, sign):
        here = pl.ds(start_of(s), rows)
        return t * cos_vm[here, :] + sign * (pltpu.roll(t, d // 2, 1) * sin_vm[here, :])

    def project(i, _):
        s = i + i // 2 - 2 * (i // 3)

        @pl.when(i == 0)
        def _():
            for c in loads[:6]:
                c.wait()

        @pl.when(i == 1)
        def _():
            for c in x_ring[:2]:
                c.wait_recv()
            for c in x_ring[4:] + dy_ring[:4]:
                c.start()
            for c in x_ring[2:4]:
                c.wait_recv()

        @pl.when(i == 3)
        def _():
            for c in x_ring[4:]:
                c.wait_recv()

        @pl.when(i > 0)
        def _():
            put(a_vm, a_out.at[0], 0).wait()

        def norm(r, _):
            some = pl.ds(pl.multiple_of(r * 16, 16), 16)
            t = x_vm[s, some, :].astype(F32)
            factor = lax.rsqrt(jnp.mean(t * t, -1, keepdims=True) + 1e-6)
            scale_s[s, some, :] = jnp.broadcast_to(factor, (16, 128))
            a_vm[some, :] = (t * factor * gain_vm[...]).astype(BF16)

        lax.fori_loop(0, rows // 16, norm, None)
        put(a_vm, a_out.at[s], 0).start()

        def tile(c, _):
            at = pl.multiple_of(c * TILE, TILE)
            t = _dot(a_vm[...], w_vm[:, pl.ds(at, TILE)], 1, 0).astype(BF16).astype(F32)
            for m in range(TILE // d):
                q_vm[s, :, pl.ds(pl.multiple_of(at + m * d, d), d)] = turn(t[:, m * d : (m + 1) * d], s, 1).astype(BF16)

        lax.fori_loop(0, width // TILE, tile, None)
        t = _dot(a_vm[...], w_vm[:, width:], 1, 0).astype(BF16)
        k_vm[pl.ds(start_of(s), rows), :] = turn(t[:, :d].astype(F32), s, 1).astype(BF16)
        v_vm[pl.ds(start_of(s), rows), :] = t[:, d:]

    lax.fori_loop(0, n, project, None)

    def heads(ref, first):
        return jnp.concatenate([ref[:, h * d : (h + 1) * d] for h in range(first, first + per)], axis=0)

    ones = jnp.ones((8, rows), BF16)

    def forward(s, _):
        top_s[...] = jnp.full_like(top_s, NEG)
        mix_s[...] = jnp.zeros_like(mix_s)

        def block(j, masked):
            here = pl.ds(pl.multiple_of(j * rows, rows), rows)
            keys = k_vm[here, :]
            values = jnp.concatenate([v_vm[here, :].T, ones], axis=0)
            scores = [_dot(keys, heads(q_vm.at[s], c * per), 1, 1) for c in range(strips)]
            weights, keeps = [], []
            for c, t in enumerate(scores):
                if masked:
                    t = jnp.where(_later(rows, STRIP, rows), t, HIDDEN)
                old = top_s[c : c + 1, :]
                top = jnp.maximum(old, t.max(axis=0, keepdims=True))
                top_s[c : c + 1, :] = top
                weights.append(jnp.exp2((t - top) * e).astype(BF16))
                keeps.append(jnp.exp2((old - top) * e))
            for c in range(strips):
                mix_s[c] = mix_s[c] * keeps[c] + _dot(values, weights[c], 1, 0)

        whole = lax.rem(me + s, n)
        lax.fori_loop(0, whole, lambda j, _: block(j, False), None)
        block(whole, True)
        for c in range(strips):
            total = mix_s[c, d : d + 1, :]
            out = (mix_s[c, :d, :] * (1 / total)).T
            lse_s[s, c : c + 1, :] = top_s[c : c + 1, :] * e + jnp.log(total) * LOG2E
            for m in range(per):
                h = c * per + m
                seen_vm[s, :, h * d : (h + 1) * d] = out[m * rows : (m + 1) * rows, :].astype(BF16)

    lax.fori_loop(0, n, forward, None)
    put(seen_vm, seen_out, 1).start()

    dk_s[...] = jnp.zeros_like(dk_s)
    dv_s[...] = jnp.zeros_like(dv_s)

    def backward(i, _):
        s = i + i // 2 - 2 * (i // 3)

        @pl.when(i == 0)
        def _():
            for c in loads[6:]:
                c.wait()
            for c in dy_ring[:2]:
                c.wait_recv()
            for c in dy_ring[4:]:
                c.start()

        @pl.when(i == 1)
        def _():
            for c in dy_ring[2:4]:
                c.wait_recv()

        @pl.when(i == 3)
        def _():
            for c in dy_ring[4:]:
                c.wait_recv()

        put(dy_vm.at[s], dy_out.at[s], 2 + s).start()

        def tile(c, _):
            at = pl.ds(pl.multiple_of(c * TILE, TILE), TILE)
            ds_vm[:, at] = _dot(dy_vm[s], wo_vm[at, :], 1, 1).astype(BF16)

        lax.fori_loop(0, width // TILE, tile, None)
        dq_s[...] = jnp.zeros_like(dq_s)
        for h in range(g):
            at = slice(h * d, (h + 1) * d)
            both = ds_vm[:, at].astype(F32) * seen_vm[s, :, at].astype(F32)
            c, m = divmod(h, per)
            delta_s[c : c + 1, m * rows : (m + 1) * rows] = both.T.sum(axis=0, keepdims=True)

        def block(j, masked):
            here = pl.ds(pl.multiple_of(j * rows, rows), rows)
            keys, values = k_vm[here, :], v_vm[here, :]
            qs = [heads(q_vm.at[s], c * per) for c in range(strips)]
            dos = [heads(ds_vm, c * per) for c in range(strips)]
            scores = [_dot(keys, t, 1, 1) for t in qs]
            dps = [_dot(values, t, 1, 1) for t in dos]
            for c in range(strips):
                p = jnp.exp2(scores[c] * e - lse_s[s, c : c + 1, :])
                if masked:
                    p = jnp.where(_later(rows, STRIP, rows), p, 0.0)
                ds = (p * (dps[c] - delta_s[c : c + 1, :])).astype(BF16)
                dv_s[here, :] += _dot(p.astype(BF16), dos[c], 1, 0)
                dk_s[here, :] += _dot(ds, qs[c], 1, 0)
                dq_s[c] += _dot(keys.T, ds, 1, 0)

        whole = lax.rem(me + s, n)
        lax.fori_loop(0, whole, lambda j, _: block(j, False), None)
        block(whole, True)
        for c in range(strips):
            dq = (dq_s[c] * scale).T
            for m in range(per):
                h = c * per + m
                dqkv_vm[s, :, h * d : (h + 1) * d] = turn(dq[m * rows : (m + 1) * rows, :], s, -1).astype(BF16)

    lax.fori_loop(0, n, backward, None)
    for s in range(n):
        here = pl.ds(start_of(s), rows)
        dqkv_vm[s, :, width : width + d] = turn(dk_s[here, :] * scale, s, -1).astype(BF16)
        dqkv_vm[s, :, width + d :] = dv_s[here, :].astype(BF16)
    put(dqkv_vm, dqkv_out, 6).start()
    for s in range(n):
        put(dy_vm.at[s], dy_out.at[s], 2 + s).wait()
    for c in x_ring + dy_ring:
        c.wait_send()

    gain_s[...] = jnp.zeros_like(gain_s)
    dots_vm[...] = jnp.zeros_like(dots_vm)
    quarter = deep // 4
    first = []
    for p in range(4):
        at = pl.ds(p * quarter, quarter)
        first += [send(dy_vm.at[2, low, at], in_vm.at[0, :, at], to_right, 12 + 2 * p),
                  send(dy_vm.at[2, high, at], in_vm.at[1, :, at], to_left, 13 + 2 * p)]

    def count(t, s, at):
        unit = x_vm[s, :, at].astype(F32) * jnp.concatenate([scale_s[s]] * (t.shape[1] // 128), axis=1)
        both = t.astype(F32) * unit
        gain_s[:, at] += both.reshape(rows // 8, 8, t.shape[1]).sum(0)
        both = both * gain_vm[:, at]
        dots_vm[s] += sum(both[:, m : m + 128] for m in range(0, t.shape[1], 128))

    def opposite(c, _):
        at = pl.ds(pl.multiple_of(c * 2 * TILE, 2 * TILE), 2 * TILE)
        t = _dot(dqkv_vm[2], w_vm[at, :], 1, 1).astype(BF16)
        dy_vm[2, :, at] = t
        for p in range(4):
            @pl.when(c == (p + 1) * (quarter // (2 * TILE)) - 1)
            def _():
                first[2 * p].start()
                first[2 * p + 1].start()

        count(t, 2, at)

    lax.fori_loop(0, deep // (2 * TILE), opposite, None)

    def others(c, _):
        at = pl.ds(pl.multiple_of(c * TILE, TILE), TILE)
        slots = (1, n - 1, 0)
        t = _dot(jnp.concatenate([dqkv_vm[s] for s in slots], axis=0), w_vm[at, :], 1, 1).astype(BF16)
        for m, s in enumerate(slots):
            dy_vm[s, :, at] = t[m * rows : (m + 1) * rows, :]
            count(t[m * rows : (m + 1) * rows, :], s, at)

    lax.fori_loop(0, deep // TILE, others, None)
    ends = [put(dy_vm.at[0], own_out, 7), put(dy_vm.at[1, high], right_b_out, 8), put(dy_vm.at[n - 1, low], left_a_out, 9), put(share_vm, share_out, 10)]
    share = gain_s[...].sum(0, keepdims=True)
    for s in range(n):
        share_vm[s, :, :deep] = share
        share_vm[s, :, deep:] = dots_vm[s].T.sum(0, keepdims=True)
    for c in ends:
        c.start()
    for c in first:
        c.wait_recv()

    def add(r, _):
        some = pl.ds(pl.multiple_of(r * 16, 16), 16)
        there = pl.ds(pl.multiple_of(half + r * 16, 16), 16)
        in_vm[0, some, :] = (dy_vm[1, some, :].astype(F32) + in_vm[0, some, :].astype(F32)).astype(BF16)
        in_vm[1, some, :] = (dy_vm[n - 1, there, :].astype(F32) + in_vm[1, some, :].astype(F32)).astype(BF16)

    lax.fori_loop(0, half // 16, add, None)
    for c in (put(in_vm.at[0], sum_a_out, 11), put(in_vm.at[1], sum_b_out, 12)):
        c.start()
        ends.append(c)
    for c in first:
        c.wait_send()
    for c in ends + [put(a_vm, a_out.at[0], 0), put(seen_vm, seen_out, 1), put(dqkv_vm, dqkv_out, 6)]:
        c.wait()


def gathered(n, x, dy, gain, wq, wk, wv, wo, cos, sin):
    rows, deep = x.shape
    width, d = wq.shape[1], wk.shape[1]
    g, half = width // d, rows // 2
    strips = g * rows // STRIP
    some = pl.BlockSpec(memory_space=pl.ANY)
    out = jax.ShapeDtypeStruct
    return pl.pallas_call(
        functools.partial(_kernel, n),
        in_specs=[some, some, pl.BlockSpec(memory_space=pltpu.VMEM)] + [some] * 6,
        out_specs=[some] * 10,
        out_shape=[out((n, rows, deep), BF16), out((n, rows, deep), BF16), out((n, rows, width), BF16), out((n, rows, width + 2 * d), BF16),
                   out((rows, deep), BF16)] + [out((half, deep), BF16)] * 4 + [out((n, 1, deep + rows), F32)],
        scratch_shapes=[
            pltpu.VMEM((n, rows, deep), BF16), pltpu.VMEM((rows, deep), BF16), pltpu.VMEM((deep, width + 2 * d), BF16),
            pltpu.VMEM((width, deep), BF16), pltpu.VMEM((n, rows, deep), BF16), pltpu.VMEM((n, rows, width), BF16),
            pltpu.VMEM((n, rows, width), BF16), pltpu.VMEM((rows, width), BF16), pltpu.VMEM((n, rows, width + 2 * d), BF16),
            pltpu.VMEM((n * rows, d), BF16), pltpu.VMEM((n * rows, d), BF16), pltpu.VMEM((n * rows, d), F32), pltpu.VMEM((n * rows, d), F32),
            pltpu.VMEM((n, strips, STRIP), F32), pltpu.VMEM((strips, STRIP), F32), pltpu.VMEM((strips, d + 8, STRIP), F32),
            pltpu.VMEM((strips, d, STRIP), F32), pltpu.VMEM((strips, STRIP), F32), pltpu.VMEM((n * rows, d), F32), pltpu.VMEM((n * rows, d), F32),
            pltpu.VMEM((n, rows, 128), F32), pltpu.VMEM((2, half, deep), BF16), pltpu.VMEM((n, 1, deep + rows), F32),
            pltpu.VMEM((1, deep), F32), pltpu.VMEM((8, deep), F32), pltpu.VMEM((n, rows, 128), F32),
            pltpu.SemaphoreType.DMA((20,)), pltpu.SemaphoreType.DMA((20,)), pltpu.SemaphoreType.DMA((8,)), pltpu.SemaphoreType.DMA((13,)),
        ],
        compiler_params=pltpu.CompilerParams(collective_id=0, has_side_effects=True, vmem_limit_bytes=VMEM),
        cost_estimate=pl.CostEstimate(flops=60 * rows * deep * width, transcendentals=0, bytes_accessed=20 * rows * deep),
    )(x, dy, gain, wq, wk, wv, wo, cos, sin)


def solution(mesh):
    n = mesh.shape["tp"]

    def step(x, dy, gain, wq, wk, wv, wo):
        rows, deep = x.shape
        width = wq.shape[1]

        half_head = HEAD // 2
        rate = np.float32(THETA) ** (-np.arange(half_head, dtype=np.float32) / np.float32(half_head))
        angle = np.arange(n * rows, dtype=np.float32)[:, None] * rate
        cos = jnp.asarray(np.concatenate([np.cos(angle)] * 2, 1))
        sin = jnp.asarray(np.concatenate([-np.sin(angle), np.sin(angle)], 1))

        normal, dy_all, seen, dqkv, own, right_b, left_a, sum_a, sum_b, share = gathered(n, x, dy, gain, wq, wk, wv, wo, cos, sin)

        def moved(t, places):
            return lax.ppermute(t, "tp", [(i, (i + places) % n) for i in range(n)])

        own_b, own_a = moved(right_b, 1), moved(left_a, -1)
        shares = [share[0]] + [moved(share[o], o) for o in range(1, n)]
        last_a, last_b = moved(sum_a, 1), moved(sum_b, -1)

        normal, dy_all, seen, dqkv = (t.reshape(n * rows, -1) for t in (normal, dy_all, seen, dqkv))
        by_wo = _dot(seen, dy_all, 0, 0).astype(BF16)
        by_wq = _dot(normal, dqkv[:, :width], 0, 0).astype(BF16)
        by_wkv = _dot(normal, dqkv[:, width:], 0, 0).astype(BF16)
        by_wk, by_wv = by_wkv[:, :HEAD], by_wkv[:, HEAD:]

        me = lax.axis_index("tp")
        shares = jnp.concatenate(shares)
        mean = shares[:, deep:].sum(0)[:, None] / deep
        by_gain = jnp.roll(shares[::-1, :deep], me + 1, axis=0).sum(0, keepdims=True)

        wide, gain = x.astype(F32), gain.astype(F32)
        scale = lax.rsqrt(jnp.mean(wide * wide, -1, keepdims=True) + 1e-6)
        most = scale * ((own.astype(F32) + jnp.concatenate([own_a, own_b]).astype(F32)) * gain - wide * scale * mean) + dy.astype(F32)
        most = lax.optimization_barrier(most)
        by_x = most + scale * gain * jnp.concatenate([last_a, last_b]).astype(F32)
        return by_x.astype(BF16), by_gain, by_wq, by_wk, by_wv, by_wo

    tokens, columns = P(("dp", "tp"), None), P(None, "tp")
    return jax.shard_map(
        step,
        mesh=mesh,
        in_specs=(tokens, tokens, P(None), columns, columns, columns, P("tp", None)),
        out_specs=(tokens, P("dp", None), P("dp", "tp"), P("dp", "tp"), P("dp", "tp"), P(("dp", "tp"), None)),
        check_vma=False,
    )
```

```python
import functools

import jax
import jax.numpy as jnp
import numpy as np
from jax import lax
from jax.experimental import pallas as pl
from jax.experimental.pallas import tpu as pltpu
from jax.sharding import PartitionSpec as P

HEAD = 128
THETA = 10000
NEG = -1e30
HIDDEN = 2 * NEG
LOG2E = 1.4426950408889634
VMEM = 67043328
STRIP = 512
TILE = 256
F32, BF16 = jnp.float32, jnp.bfloat16


def _dot(a, b, ca, cb):
    return lax.dot_general(a, b, (((ca,), (cb,)), ((), ())), preferred_element_type=F32)


def _later(bk, cols, bq):
    return lax.rem(lax.broadcasted_iota(jnp.int32, (bk, cols), 1), bq) >= lax.broadcasted_iota(jnp.int32, (bk, cols), 0)


def _kernel(n, x_ref, dy_ref, gain_ref, wq_ref, wk_ref, wv_ref, wo_ref, table_ref,
            a_out, dy_out, seen_out, dqkv_out, own_out, right_b_out, left_a_out, sum_a_out, sum_b_out, share_out,
            x_vm, w_vm, wo_vm, dy_vm, q_vm, seen_vm, ds_vm, dqkv_vm, k_vm, v_vm, dk_s, dv_s, lse_s, top_s, mix_s, delta_s,
            cos_vm, sin_vm, scale_s, in_vm, share_vm, shares_vm, gain_vm, gain_s, dots_vm, p_vm, acc_s, send_sem, recv_sem, load_sem, out_sem):
    rows, deep = x_ref.shape
    half = rows // 2
    d = k_vm.shape[1]
    dq_s, a_vm = mix_s.at[:, :d, :], in_vm
    width = wq_ref.shape[1]
    g = width // d
    per = STRIP // rows
    strips = g // per
    scale = d**-0.5
    e = scale * LOG2E
    me = lax.axis_index("tp")
    to_right, to_left = lax.rem(me + 1, n), lax.rem(me + n - 1, n)
    low, high = pl.ds(0, half), pl.ds(half, half)

    def start_of(s):
        return pl.multiple_of(lax.rem(me + s, n) * rows, rows)

    def send(src, dst, to, i):
        return pltpu.make_async_remote_copy(src_ref=src, dst_ref=dst, send_sem=send_sem.at[i], recv_sem=recv_sem.at[i],
                                            device_id={"tp": to}, device_id_type=pl.DeviceIdType.MESH)

    def load(src, dst, i):
        return pltpu.make_async_copy(src, dst, load_sem.at[i])

    def put(src, dst, i):
        return pltpu.make_async_copy(src, dst, out_sem.at[i])

    def ring(own, at, i):
        return [send(own.at[low], at.at[n - 1, low], to_right, i), send(own.at[high], at.at[1, high], to_left, i + 1),
                send(own.at[high], at.at[n - 1, high], to_right, i + 2), send(own.at[low], at.at[1, low], to_left, i + 3),
                send(at.at[n - 1, low], at.at[2, low], to_right, i + 4), send(at.at[1, high], at.at[2, high], to_left, i + 5)]

    quarter, eighth = deep // 4, deep // 8

    def far(q):
        at = pl.ds(pl.multiple_of(q * quarter, quarter), quarter)
        return [send(dy_vm.at[n - 1, low, at], dy_vm.at[2, low, at], to_right, 10 + 2 * q),
                send(dy_vm.at[1, high, at], dy_vm.at[2, high, at], to_left, 11 + 2 * q)]

    x_ring, dy_ring = ring(x_ref, x_vm, 0), ring(dy_ref, dy_vm, 6)[:4]
    loads = [load(x_ref, x_vm.at[0], 0), load(wq_ref, w_vm.at[:, pl.ds(0, width)], 1), load(wk_ref, w_vm.at[:, pl.ds(width, d)], 2),
             load(wv_ref, w_vm.at[:, pl.ds(width + d, d)], 3), load(table_ref, cos_vm, 4), load(dy_ref, dy_vm.at[0], 5), load(wo_ref, wo_vm, 6)]

    barrier = pltpu.get_barrier_semaphore()
    for o in range(1, n):
        pl.semaphore_signal(barrier, inc=1, device_id={"tp": lax.rem(me + o, n)}, device_id_type=pl.DeviceIdType.MESH)
    pl.semaphore_wait(barrier, n - 1)
    for c in x_ring[:4]:
        c.start()
    for c in loads:
        c.start()

    gain_vm[...] = gain_ref[...].astype(F32).reshape(1, deep)

    def turn(t, s, sign):
        here = pl.ds(start_of(s), rows)
        return t * cos_vm[here, :] + sign * (pltpu.roll(t, d // 2, 1) * sin_vm[here, :])

    def project(i, _):
        s = i + i // 2 - 2 * (i // 3)

        @pl.when(i == 0)
        def _():
            for c in loads[:5]:
                c.wait()
            table = cos_vm[...]
            other = pltpu.roll(table, d // 2, 1)
            left_half = lax.broadcasted_iota(jnp.int32, table.shape, 1) < d // 2
            cos_vm[...] = jnp.where(left_half, table, other)
            sin_vm[...] = jnp.where(left_half, -other, table)

        @pl.when(i == 1)
        def _():
            for c in x_ring[:2]:
                c.wait_recv()
            for c in x_ring[4:] + dy_ring[:4]:
                c.start()
            for c in x_ring[2:4]:
                c.wait_recv()

        @pl.when(i == 3)
        def _():
            for c in x_ring[4:]:
                c.wait_recv()

        @pl.when(i > 0)
        def _():
            put(a_vm, a_out.at[0], 0).wait()

        def norm(r, _):
            some = pl.ds(pl.multiple_of(r * 16, 16), 16)
            t = x_vm[s, some, :].astype(F32)
            factor = lax.rsqrt(jnp.mean(t * t, -1, keepdims=True) + 1e-6)
            scale_s[s, some, :] = jnp.broadcast_to(factor, (16, 128))
            a_vm[r // (half // 16), pl.ds(pl.multiple_of(lax.rem(r * 16, half), 16), 16), :] = (t * factor * gain_vm[...]).astype(BF16)

        lax.fori_loop(0, rows // 16, norm, None)
        put(a_vm, a_out.at[s], 0).start()

        def tile(c, _):
            at = pl.multiple_of(c * TILE, TILE)
            t = _dot(a_vm[...].reshape(rows, deep), w_vm[:, pl.ds(at, TILE)], 1, 0).astype(BF16).astype(F32)
            for m in range(TILE // d):
                q_vm[s, :, pl.ds(pl.multiple_of(at + m * d, d), d)] = turn(t[:, m * d : (m + 1) * d], s, 1).astype(BF16)

        lax.fori_loop(0, width // TILE, tile, None)
        t = _dot(a_vm[...].reshape(rows, deep), w_vm[:, width:], 1, 0).astype(BF16)
        k_vm[pl.ds(start_of(s), rows), :] = turn(t[:, :d].astype(F32), s, 1).astype(BF16)
        v_vm[pl.ds(start_of(s), rows), :] = t[:, d:]

    lax.fori_loop(0, n, project, None)

    def heads(ref, first):
        return jnp.concatenate([ref[:, h * d : (h + 1) * d] for h in range(first, first + per)], axis=0)

    ones = jnp.ones((8, rows), BF16)

    def forward(s, _):
        top_s[...] = jnp.full_like(top_s, NEG)
        mix_s[...] = jnp.zeros_like(mix_s)

        def block(j, masked):
            here = pl.ds(pl.multiple_of(j * rows, rows), rows)
            keys = k_vm[here, :]
            values = jnp.concatenate([v_vm[here, :].T, ones], axis=0)
            scores = [_dot(keys, heads(q_vm.at[s], c * per), 1, 1) for c in range(strips)]
            weights, keeps = [], []
            for c, t in enumerate(scores):
                if masked:
                    t = jnp.where(_later(rows, STRIP, rows), t, HIDDEN)
                old = top_s[c : c + 1, :]
                top = jnp.maximum(old, t.max(axis=0, keepdims=True))
                top_s[c : c + 1, :] = top
                weights.append(jnp.exp2((t - top) * e).astype(BF16))
                keeps.append(jnp.exp2((old - top) * e))
            for c in range(strips):
                mix_s[c] = mix_s[c] * keeps[c] + _dot(values, weights[c], 1, 0)

        whole = lax.rem(me + s, n)
        lax.fori_loop(0, whole, lambda j, _: block(j, False), None)
        block(whole, True)
        for c in range(strips):
            total = mix_s[c, d : d + 1, :]
            out = (mix_s[c, :d, :] * (1 / total)).T
            lse_s[s, c : c + 1, :] = top_s[c : c + 1, :] * e + jnp.log(total) * LOG2E
            for m in range(per):
                h = c * per + m
                seen_vm[s, :, h * d : (h + 1) * d] = out[m * rows : (m + 1) * rows, :].astype(BF16)

    lax.fori_loop(0, n, forward, None)
    put(seen_vm, seen_out, 1).start()

    dk_s[...] = jnp.zeros_like(dk_s)
    dv_s[...] = jnp.zeros_like(dv_s)

    def delta(s):
        for h in range(g):
            at = slice(h * d, (h + 1) * d)
            both = ds_vm[:, at].astype(F32) * seen_vm[s, :, at].astype(F32)
            c, m = divmod(h, per)
            delta_s[c : c + 1, m * rows : (m + 1) * rows] = both.T.sum(axis=0, keepdims=True)

    def weigh(s, c, scores, masked):
        p = jnp.exp2(scores * e - lse_s[s, c : c + 1, :])
        return (jnp.where(_later(rows, STRIP, rows), p, 0.0) if masked else p).astype(BF16)

    def back(s, j, weights):
        here = pl.ds(pl.multiple_of(j * rows, rows), rows)
        keys, values = k_vm[here, :], v_vm[here, :]
        qs = [heads(q_vm.at[s], c * per) for c in range(strips)]
        dos = [heads(ds_vm, c * per) for c in range(strips)]
        ps = weights(keys, qs)
        dps = [_dot(values, t, 1, 1) for t in dos]
        for c in range(strips):
            p = ps(c)
            ds = (p.astype(F32) * (dps[c] - delta_s[c : c + 1, :])).astype(BF16)
            dv_s[here, :] += _dot(p, dos[c], 1, 0)
            dk_s[here, :] += _dot(ds, qs[c], 1, 0)
            dq_s[c] += _dot(keys.T, ds, 1, 0)

    def dq_out(s):
        for c in range(strips):
            dq = (dq_s[c] * scale).T
            for m in range(per):
                h = c * per + m
                dqkv_vm[s, :, h * d : (h + 1) * d] = turn(dq[m * rows : (m + 1) * rows, :], s, -1).astype(BF16)

    def near(i, _):
        s = i + i // 2

        @pl.when(i == 0)
        def _():
            put(a_vm, a_out.at[0], 0).wait()
            for c in loads[5:]:
                c.wait()
            for c in dy_ring[:2]:
                c.wait_recv()
            for q in range(4):
                for c in far(q):
                    c.start()

        @pl.when(i == 1)
        def _():
            for c in dy_ring[2:]:
                c.wait_recv()

        put(dy_vm.at[s], dy_out.at[s], 2 + s).start()

        def tile(c, _):
            at = pl.ds(pl.multiple_of(c * TILE, TILE), TILE)
            ds_vm[:, at] = _dot(dy_vm[s], wo_vm[at, :], 1, 1).astype(BF16)

        lax.fori_loop(0, width // TILE, tile, None)
        dq_s[...] = jnp.zeros_like(dq_s)
        delta(s)

        def fresh(masked):
            def weights(keys, qs):
                scores = [_dot(keys, t, 1, 1) for t in qs]
                return lambda c: weigh(s, c, scores[c], masked)
            return weights

        whole = lax.rem(me + s, n)
        lax.fori_loop(0, whole, lambda j, _: back(s, j, fresh(False)), None)
        back(s, whole, fresh(True))
        dq_out(s)

    lax.fori_loop(0, n - 1, near, None)

    whole = lax.rem(me + 2, n)

    def ahead(j, masked):
        keys = k_vm[pl.ds(pl.multiple_of(j * rows, rows), rows), :]
        for c in range(strips):
            p_vm[j, c] = weigh(2, c, _dot(keys, heads(q_vm.at[2], c * per), 1, 1), masked)

    lax.fori_loop(0, whole, lambda j, _: ahead(j, False), None)
    ahead(whole, True)
    dq_s[...] = jnp.zeros_like(dq_s)
    gain_s[...] = jnp.zeros_like(gain_s)
    dots_vm[...] = jnp.zeros_like(dots_vm)
    acc_s[...] = jnp.zeros_like(acc_s)

    def through(q, _):
        for c in far(q):
            c.wait_recv()
        part = pl.ds(pl.multiple_of(q * quarter, quarter), quarter)

        def tile(c, _):
            at = pl.ds(pl.multiple_of(c * TILE, TILE), TILE)
            acc_s[:, at] += _dot(dy_vm[2, :, part], wo_vm[at, part], 1, 1)

        lax.fori_loop(0, width // TILE, tile, None)

    lax.fori_loop(0, 4, through, None)
    put(dy_vm.at[2], dy_out.at[2], 4).start()
    ds_vm[...] = acc_s[...].astype(BF16)
    delta(2)
    lax.fori_loop(0, whole + 1, lambda j, _: back(2, j, lambda keys, qs: lambda c: p_vm[j, c]), None)
    dq_out(2)

    def dkv_out(s):
        here = pl.ds(start_of(s), rows)
        dqkv_vm[s, :, width : width + d] = turn(dk_s[here, :] * scale, s, -1).astype(BF16)
        dqkv_vm[s, :, width + d :] = dv_s[here, :].astype(BF16)

    dkv_out(2)
    put(dy_vm.at[2], dy_out.at[2], 4).wait()

    def first(p):
        at = pl.ds(pl.multiple_of(p * eighth, eighth), eighth)
        return [send(dy_vm.at[2, low, at], in_vm.at[0, :, at], to_right, 18 + 2 * p), send(dy_vm.at[2, high, at], in_vm.at[1, :, at], to_left, 19 + 2 * p)]

    def count(t, s, at):
        unit = x_vm[s, :, at].astype(F32) * jnp.concatenate([scale_s[s]] * (t.shape[1] // 128), axis=1)
        both = t.astype(F32) * unit
        gain_s[:, at] += both.reshape(rows // 8, 8, t.shape[1]).sum(0)
        both = both * gain_vm[:, at]
        dots_vm[s] += sum(both[:, m : m + 128] for m in range(0, t.shape[1], 128))

    def opposite(c, _):
        at = pl.ds(pl.multiple_of(c * eighth, eighth), eighth)
        t = _dot(dqkv_vm[2], w_vm[at, :], 1, 1).astype(BF16)
        dy_vm[2, :, at] = t

        @pl.when(c < 7)
        def _():
            for k in first(c):
                k.start()

        count(t, 2, at)

    lax.fori_loop(0, 8, opposite, None)
    for s in (0, 1, n - 1):
        dkv_out(s)
        put(dy_vm.at[s], dy_out.at[s], 2 + s).wait()
    put(dqkv_vm, dqkv_out, 6).start()
    for c in x_ring + dy_ring + [c for q in range(4) for c in far(q)]:
        c.wait_send()

    def others(c, _):
        at = pl.ds(pl.multiple_of(c * TILE, TILE), TILE)
        slots = (1, n - 1, 0)
        t = _dot(jnp.concatenate([dqkv_vm[s] for s in slots], axis=0), w_vm[at, :], 1, 1).astype(BF16)
        for m, s in enumerate(slots):
            dy_vm[s, :, at] = t[m * rows : (m + 1) * rows, :]
            count(t[m * rows : (m + 1) * rows, :], s, at)

    lax.fori_loop(0, deep // TILE, others, None)
    share = gain_s[...].sum(0, keepdims=True)
    for s in range(n):
        share_vm[s, :, :deep] = share
        share_vm[s, :, deep:] = dots_vm[s].T.sum(0, keepdims=True)
    shares_vm[me] = share_vm[0]
    shares = [send(share_vm.at[o], shares_vm.at[me], lax.rem(me + o, n), 33 + o) for o in range(1, n)]
    for c in shares + first(7):
        c.start()
    ends = [put(dy_vm.at[0], own_out, 7), put(dy_vm.at[1, high], right_b_out, 8), put(dy_vm.at[n - 1, low], left_a_out, 9), put(shares_vm, share_out, 10)]
    for c in ends[:3]:
        c.start()

    def sums(p):
        at = pl.ds(pl.multiple_of(p * eighth, eighth), eighth)
        return [put(in_vm.at[0, :, at], sum_a_out.at[:, at], 14 + 2 * p), put(in_vm.at[1, :, at], sum_b_out.at[:, at], 15 + 2 * p)]

    def add(p, _):
        at = pl.ds(pl.multiple_of(p * eighth, eighth), eighth)
        for c in first(p):
            c.wait_recv()
        in_vm[0, :, at] = (dy_vm[1, :half, at].astype(F32) + in_vm[0, :, at].astype(F32)).astype(BF16)
        in_vm[1, :, at] = (dy_vm[n - 1, half:, at].astype(F32) + in_vm[1, :, at].astype(F32)).astype(BF16)
        for c in sums(p):
            c.start()

    lax.fori_loop(0, 7, add, None)
    for c in shares:
        c.wait_recv()
    ends[3].start()
    add(7, None)
    for c in shares:
        c.wait_send()
    for p in range(8):
        for c in first(p):
            c.wait_send()
        ends += sums(p)
    for c in ends + [put(seen_vm, seen_out, 1), put(dqkv_vm, dqkv_out, 6)]:
        c.wait()


def gathered(n, x, dy, gain, wq, wk, wv, wo, table):
    rows, deep = x.shape
    width, d = wq.shape[1], wk.shape[1]
    g, half = width // d, rows // 2
    strips = g * rows // STRIP
    some = pl.BlockSpec(memory_space=pl.ANY)
    out = jax.ShapeDtypeStruct
    return pl.pallas_call(
        functools.partial(_kernel, n),
        in_specs=[some, some, pl.BlockSpec(memory_space=pltpu.VMEM)] + [some] * 5,
        out_specs=[some] * 10,
        out_shape=[out((n, 2, half, deep), BF16), out((n, rows, deep), BF16), out((n, rows, width), BF16), out((n, rows, width + 2 * d), BF16),
                   out((rows, deep), BF16)] + [out((half, deep), BF16)] * 4 + [out((n, 1, deep + rows), F32)],
        scratch_shapes=[
            pltpu.VMEM((n, rows, deep), BF16), pltpu.VMEM((deep, width + 2 * d), BF16),
            pltpu.VMEM((width, deep), BF16), pltpu.VMEM((n, rows, deep), BF16), pltpu.VMEM((n, rows, width), BF16),
            pltpu.VMEM((n, rows, width), BF16), pltpu.VMEM((rows, width), BF16), pltpu.VMEM((n, rows, width + 2 * d), BF16),
            pltpu.VMEM((n * rows, d), BF16), pltpu.VMEM((n * rows, d), BF16), pltpu.VMEM((n * rows, d), F32), pltpu.VMEM((n * rows, d), F32),
            pltpu.VMEM((n, strips, STRIP), F32), pltpu.VMEM((strips, STRIP), F32), pltpu.VMEM((strips, d + 8, STRIP), F32),
            pltpu.VMEM((strips, STRIP), F32), pltpu.VMEM((n * rows, d), F32), pltpu.VMEM((n * rows, d), F32),
            pltpu.VMEM((n, rows, 128), F32), pltpu.VMEM((2, half, deep), BF16), pltpu.VMEM((n, 1, deep + rows), F32), pltpu.VMEM((n, 1, deep + rows), F32),
            pltpu.VMEM((1, deep), F32), pltpu.VMEM((8, deep), F32), pltpu.VMEM((n, rows, 128), F32),
            pltpu.VMEM((n, strips, rows, STRIP), BF16), pltpu.VMEM((rows, width), F32),
            pltpu.SemaphoreType.DMA((37,)), pltpu.SemaphoreType.DMA((37,)), pltpu.SemaphoreType.DMA((7,)), pltpu.SemaphoreType.DMA((30,)),
        ],
        compiler_params=pltpu.CompilerParams(collective_id=0, has_side_effects=True, vmem_limit_bytes=VMEM),
        cost_estimate=pl.CostEstimate(flops=60 * rows * deep * width, transcendentals=0, bytes_accessed=20 * rows * deep),
    )(x, dy, gain, wq, wk, wv, wo, table)


def solution(mesh):
    n = mesh.shape["tp"]

    def step(x, dy, gain, wq, wk, wv, wo):
        rows, deep = x.shape
        width = wq.shape[1]

        half_head = HEAD // 2
        rate = np.float32(THETA) ** (-np.arange(half_head, dtype=np.float32) / np.float32(half_head))
        angle = np.arange(n * rows, dtype=np.float32)[:, None] * rate
        table = jnp.asarray(np.concatenate([np.cos(angle), np.sin(angle)], 1))

        normal, dy_all, seen, dqkv, own, right_b, left_a, sum_a, sum_b, shares = gathered(n, x, dy, gain, wq, wk, wv, wo, table)

        def moved(t, places):
            return lax.ppermute(t, "tp", [(i, (i + places) % n) for i in range(n)])

        own_b, own_a = moved(right_b, 1), moved(left_a, -1)
        last_a, last_b = moved(sum_a, 1), moved(sum_b, -1)

        normal, dy_all, seen, dqkv = (t.reshape(n * rows, -1) for t in (normal, dy_all, seen, dqkv))
        by_wo = _dot(seen, dy_all, 0, 0).astype(BF16)
        by_wq = _dot(normal, dqkv[:, :width], 0, 0).astype(BF16)
        by_wkv = _dot(normal, dqkv[:, width:], 0, 0).astype(BF16)
        by_wk, by_wv = by_wkv[:, :HEAD], by_wkv[:, HEAD:]

        shares = shares.sum((0, 1))
        by_gain, mean = shares[None, :deep], shares[deep:, None] / deep

        wide, gain = x.astype(F32), gain.astype(F32)
        scale = lax.rsqrt(jnp.mean(wide * wide, -1, keepdims=True) + 1e-6)
        most = scale * ((own.astype(F32) + jnp.concatenate([own_a, own_b]).astype(F32)) * gain - wide * scale * mean) + dy.astype(F32)
        most = lax.optimization_barrier(most)
        by_x = most + scale * gain * jnp.concatenate([last_a, last_b]).astype(F32)
        return by_x.astype(BF16), by_gain, by_wq, by_wk, by_wv, by_wo

    tokens, columns = P(("dp", "tp"), None), P(None, "tp")
    return jax.shard_map(
        step,
        mesh=mesh,
        in_specs=(tokens, tokens, P(None), columns, columns, columns, P("tp", None)),
        out_specs=(tokens, P("dp", None), P("dp", "tp"), P("dp", "tp"), P("dp", "tp"), P(("dp", "tp"), None)),
        check_vma=False,
    )
```

```python
import functools

import jax
import jax.numpy as jnp
import numpy as np
from jax import lax
from jax.experimental import pallas as pl
from jax.experimental.pallas import tpu as pltpu
from jax.sharding import PartitionSpec as P

HEAD = 128
THETA = 10000
NEG = -1e30
HIDDEN = 2 * NEG
LOG2E = 1.4426950408889634
VMEM = 67043328
STRIP = 512
TILE = 256
F32, BF16 = jnp.float32, jnp.bfloat16


def _dot(a, b, ca, cb):
    return lax.dot_general(a, b, (((ca,), (cb,)), ((), ())), preferred_element_type=F32)


def _later(bk, cols, bq):
    return lax.rem(lax.broadcasted_iota(jnp.int32, (bk, cols), 1), bq) >= lax.broadcasted_iota(jnp.int32, (bk, cols), 0)


def _kernel(n, x_ref, dy_ref, gain_ref, wq_ref, wk_ref, wv_ref, wo_ref, table_ref,
            a_out, dy_out, seen_out, dqkv_out, own_out, right_b_out, left_a_out, sum_a_out, sum_b_out, share_out,
            x_vm, w_vm, wo_vm, dy_vm, q_vm, seen_vm, ds_vm, dqkv_vm, k_vm, v_vm, dk_s, dv_s, lse_s, top_s, mix_s, delta_s,
            cos_vm, sin_vm, scale_s, in_vm, share_vm, shares_vm, gain_vm, gain_s, dots_vm, p_vm, acc_s, send_sem, recv_sem, load_sem, out_sem):
    rows, deep = x_ref.shape
    half = rows // 2
    d = k_vm.shape[1]
    dq_s, a_vm = mix_s.at[:, :d, :], in_vm
    width = wq_ref.shape[1]
    g = width // d
    per = STRIP // rows
    strips = g // per
    scale = d**-0.5
    e = scale * LOG2E
    me = lax.axis_index("tp")
    to_right, to_left = lax.rem(me + 1, n), lax.rem(me + n - 1, n)
    low, high = pl.ds(0, half), pl.ds(half, half)

    def start_of(s):
        return pl.multiple_of(lax.rem(me + s, n) * rows, rows)

    def send(src, dst, to, i):
        return pltpu.make_async_remote_copy(src_ref=src, dst_ref=dst, send_sem=send_sem.at[i], recv_sem=recv_sem.at[i],
                                            device_id={"tp": to}, device_id_type=pl.DeviceIdType.MESH)

    def load(src, dst, i):
        return pltpu.make_async_copy(src, dst, load_sem.at[i])

    def put(src, dst, i):
        return pltpu.make_async_copy(src, dst, out_sem.at[i])

    def ring(own, at, i):
        return [send(own.at[low], at.at[n - 1, low], to_right, i), send(own.at[high], at.at[1, high], to_left, i + 1),
                send(own.at[high], at.at[n - 1, high], to_right, i + 2), send(own.at[low], at.at[1, low], to_left, i + 3),
                send(at.at[n - 1, low], at.at[2, low], to_right, i + 4), send(at.at[1, high], at.at[2, high], to_left, i + 5)]

    quarter, eighth = deep // 4, deep // 8

    def far(q):
        at = pl.ds(pl.multiple_of(q * quarter, quarter), quarter)
        return [send(dy_vm.at[n - 1, low, at], dy_vm.at[2, low, at], to_right, 10 + 2 * q),
                send(dy_vm.at[1, high, at], dy_vm.at[2, high, at], to_left, 11 + 2 * q)]

    x_ring, dy_ring = ring(x_ref, x_vm, 0), ring(dy_ref, dy_vm, 6)[:4]
    loads = [load(x_ref, x_vm.at[0], 0), load(wq_ref, w_vm.at[:, pl.ds(0, width)], 1), load(wk_ref, w_vm.at[:, pl.ds(width, d)], 2),
             load(wv_ref, w_vm.at[:, pl.ds(width + d, d)], 3), load(table_ref, cos_vm, 4), load(dy_ref, dy_vm.at[0], 5), load(wo_ref, wo_vm, 6)]

    barrier = pltpu.get_barrier_semaphore()
    for o in range(1, n):
        pl.semaphore_signal(barrier, inc=1, device_id={"tp": lax.rem(me + o, n)}, device_id_type=pl.DeviceIdType.MESH)
    pl.semaphore_wait(barrier, n - 1)
    for c in x_ring[:4]:
        c.start()
    for c in loads:
        c.start()

    gain_vm[...] = gain_ref[...].astype(F32).reshape(1, deep)

    def turn(t, s, sign):
        here = pl.ds(start_of(s), rows)
        return t * cos_vm[here, :] + sign * (pltpu.roll(t, d // 2, 1) * sin_vm[here, :])

    def project(i, _):
        s = i + i // 2 - 2 * (i // 3)

        @pl.when(i == 0)
        def _():
            for c in loads[:5]:
                c.wait()
            table = cos_vm[...]
            other = pltpu.roll(table, d // 2, 1)
            left_half = lax.broadcasted_iota(jnp.int32, table.shape, 1) < d // 2
            cos_vm[...] = jnp.where(left_half, table, other)
            sin_vm[...] = jnp.where(left_half, -other, table)

        @pl.when(i == 1)
        def _():
            for c in x_ring[:2]:
                c.wait_recv()
            for c in x_ring[4:] + dy_ring[:4]:
                c.start()
            for c in x_ring[2:4]:
                c.wait_recv()

        @pl.when(i == 3)
        def _():
            for c in x_ring[4:]:
                c.wait_recv()

        @pl.when(i > 0)
        def _():
            put(a_vm, a_out.at[0], 0).wait()

        def norm(r, _):
            some = pl.ds(pl.multiple_of(r * 16, 16), 16)
            t = x_vm[s, some, :].astype(F32)
            factor = lax.rsqrt(jnp.mean(t * t, -1, keepdims=True) + 1e-6)
            scale_s[s, some, :] = jnp.broadcast_to(factor, (16, 128))
            a_vm[r // (half // 16), pl.ds(pl.multiple_of(lax.rem(r * 16, half), 16), 16), :] = (t * factor * gain_vm[...]).astype(BF16)

        lax.fori_loop(0, rows // 16, norm, None)
        put(a_vm, a_out.at[s], 0).start()

        def tile(c, _):
            at = pl.multiple_of(c * TILE, TILE)
            t = _dot(a_vm[...].reshape(rows, deep), w_vm[:, pl.ds(at, TILE)], 1, 0).astype(BF16).astype(F32)
            for m in range(TILE // d):
                q_vm[s, :, pl.ds(pl.multiple_of(at + m * d, d), d)] = turn(t[:, m * d : (m + 1) * d], s, 1).astype(BF16)

        lax.fori_loop(0, width // TILE, tile, None)
        t = _dot(a_vm[...].reshape(rows, deep), w_vm[:, width:], 1, 0).astype(BF16)
        k_vm[pl.ds(start_of(s), rows), :] = turn(t[:, :d].astype(F32), s, 1).astype(BF16)
        v_vm[pl.ds(start_of(s), rows), :] = t[:, d:]

    lax.fori_loop(0, n, project, None)

    def heads(ref, first):
        return jnp.concatenate([ref[:, h * d : (h + 1) * d] for h in range(first, first + per)], axis=0)

    ones = jnp.ones((8, rows), BF16)

    def forward(s, _):
        top_s[...] = jnp.full_like(top_s, NEG)
        mix_s[...] = jnp.zeros_like(mix_s)

        def block(j, masked):
            here = pl.ds(pl.multiple_of(j * rows, rows), rows)
            keys = k_vm[here, :]
            values = jnp.concatenate([v_vm[here, :].T, ones], axis=0)
            scores = [_dot(keys, heads(q_vm.at[s], c * per), 1, 1) for c in range(strips)]
            weights, keeps = [], []
            for c, t in enumerate(scores):
                if masked:
                    t = jnp.where(_later(rows, STRIP, rows), t, HIDDEN)
                old = top_s[c : c + 1, :]
                top = jnp.maximum(old, t.max(axis=0, keepdims=True))
                top_s[c : c + 1, :] = top
                weights.append(jnp.exp2((t - top) * e).astype(BF16))
                keeps.append(jnp.exp2((old - top) * e))
            for c in range(strips):
                mix_s[c] = mix_s[c] * keeps[c] + _dot(values, weights[c], 1, 0)

        whole = lax.rem(me + s, n)
        lax.fori_loop(0, whole, lambda j, _: block(j, False), None)
        block(whole, True)
        for c in range(strips):
            total = mix_s[c, d : d + 1, :]
            out = (mix_s[c, :d, :] * (1 / total)).T
            lse_s[s, c : c + 1, :] = top_s[c : c + 1, :] * e + jnp.log(total) * LOG2E
            for m in range(per):
                h = c * per + m
                seen_vm[s, :, h * d : (h + 1) * d] = out[m * rows : (m + 1) * rows, :].astype(BF16)

    lax.fori_loop(0, n, forward, None)
    put(seen_vm, seen_out, 1).start()

    dk_s[...] = jnp.zeros_like(dk_s)
    dv_s[...] = jnp.zeros_like(dv_s)

    def delta(s):
        for h in range(g):
            at = slice(h * d, (h + 1) * d)
            both = ds_vm[:, at].astype(F32) * seen_vm[s, :, at].astype(F32)
            c, m = divmod(h, per)
            delta_s[c : c + 1, m * rows : (m + 1) * rows] = both.T.sum(axis=0, keepdims=True)

    def weigh(s, c, scores, masked):
        p = jnp.exp2(scores * e - lse_s[s, c : c + 1, :])
        return jnp.where(_later(rows, STRIP, rows), p, 0.0) if masked else p

    def fresh(s, masked):
        def weights(keys, qs):
            scores = [_dot(keys, t, 1, 1) for t in qs]
            return lambda c: weigh(s, c, scores[c], masked)
        return weights

    def back(s, j, weights):
        here = pl.ds(pl.multiple_of(j * rows, rows), rows)
        keys, values = k_vm[here, :], v_vm[here, :]
        qs = [heads(q_vm.at[s], c * per) for c in range(strips)]
        dos = [heads(ds_vm, c * per) for c in range(strips)]
        ps = weights(keys, qs)
        dps = [_dot(values, t, 1, 1) for t in dos]
        for c in range(strips):
            p = ps(c)
            ds = (p * (dps[c] - delta_s[c : c + 1, :])).astype(BF16)
            dv_s[here, :] += _dot(p.astype(BF16), dos[c], 1, 0)
            dk_s[here, :] += _dot(ds, qs[c], 1, 0)
            dq_s[c] += _dot(keys.T, ds, 1, 0)

    def dq_out(s):
        for c in range(strips):
            dq = (dq_s[c] * scale).T
            for m in range(per):
                h = c * per + m
                dqkv_vm[s, :, h * d : (h + 1) * d] = turn(dq[m * rows : (m + 1) * rows, :], s, -1).astype(BF16)

    def near(i, _):
        s = i + i // 2

        @pl.when(i == 0)
        def _():
            put(a_vm, a_out.at[0], 0).wait()
            for c in loads[5:]:
                c.wait()
            for c in dy_ring[:2]:
                c.wait_recv()
            for q in range(4):
                for c in far(q):
                    c.start()

        @pl.when(i == 1)
        def _():
            for c in dy_ring[2:]:
                c.wait_recv()

        put(dy_vm.at[s], dy_out.at[s], 2 + s).start()

        def tile(c, _):
            at = pl.ds(pl.multiple_of(c * TILE, TILE), TILE)
            ds_vm[:, at] = _dot(dy_vm[s], wo_vm[at, :], 1, 1).astype(BF16)

        lax.fori_loop(0, width // TILE, tile, None)
        dq_s[...] = jnp.zeros_like(dq_s)
        delta(s)

        whole = lax.rem(me + s, n)
        lax.fori_loop(0, whole, lambda j, _: back(s, j, fresh(s, False)), None)
        back(s, whole, fresh(s, True))
        dq_out(s)

    lax.fori_loop(0, n - 1, near, None)

    whole = lax.rem(me + 2, n)

    def ahead(k, masked):
        keys = k_vm[pl.ds(pl.multiple_of((whole - k) * rows, rows), rows), :]
        for c in range(strips):
            p_vm[k, c] = weigh(2, c, _dot(keys, heads(q_vm.at[2], c * per), 1, 1), masked)

    ahead(0, True)
    lax.fori_loop(1, jnp.minimum(whole, 1) + 1, lambda k, _: ahead(k, False), None)
    dq_s[...] = jnp.zeros_like(dq_s)
    gain_s[...] = jnp.zeros_like(gain_s)
    dots_vm[...] = jnp.zeros_like(dots_vm)
    acc_s[...] = jnp.zeros_like(acc_s)

    def through(q, _):
        for c in far(q):
            c.wait_recv()
        part = pl.ds(pl.multiple_of(q * quarter, quarter), quarter)

        def tile(c, _):
            at = pl.ds(pl.multiple_of(c * TILE, TILE), TILE)
            acc_s[:, at] += _dot(dy_vm[2, :, part], wo_vm[at, part], 1, 1)

        lax.fori_loop(0, width // TILE, tile, None)

    lax.fori_loop(0, 4, through, None)
    put(dy_vm.at[2], dy_out.at[2], 4).start()
    ds_vm[...] = acc_s[...].astype(BF16)
    delta(2)
    lax.fori_loop(0, whole - 1, lambda j, _: back(2, j, fresh(2, False)), None)
    lax.fori_loop(0, jnp.minimum(whole, 1) + 1, lambda k, _: back(2, whole - k, lambda keys, qs: lambda c: p_vm[k, c]), None)
    dq_out(2)

    def dkv_out(s):
        here = pl.ds(start_of(s), rows)
        dqkv_vm[s, :, width : width + d] = turn(dk_s[here, :] * scale, s, -1).astype(BF16)
        dqkv_vm[s, :, width + d :] = dv_s[here, :].astype(BF16)

    dkv_out(2)
    put(dy_vm.at[2], dy_out.at[2], 4).wait()

    def first(p):
        at = pl.ds(pl.multiple_of(p * eighth, eighth), eighth)
        return [send(dy_vm.at[2, low, at], in_vm.at[0, :, at], to_right, 18 + 2 * p), send(dy_vm.at[2, high, at], in_vm.at[1, :, at], to_left, 19 + 2 * p)]

    def count(t, s, at):
        unit = x_vm[s, :, at].astype(F32) * jnp.concatenate([scale_s[s]] * (t.shape[1] // 128), axis=1)
        both = t.astype(F32) * unit
        gain_s[:, at] += both.reshape(rows // 8, 8, t.shape[1]).sum(0)
        both = both * gain_vm[:, at]
        dots_vm[s] += sum(both[:, m : m + 128] for m in range(0, t.shape[1], 128))

    def opposite(c, _):
        at = pl.ds(pl.multiple_of(c * eighth, eighth), eighth)
        t = _dot(dqkv_vm[2], w_vm[at, :], 1, 1).astype(BF16)
        dy_vm[2, :, at] = t

        @pl.when(c < 7)
        def _():
            for k in first(c):
                k.start()

        count(t, 2, at)

    lax.fori_loop(0, 8, opposite, None)
    for s in (0, 1, n - 1):
        dkv_out(s)
        put(dy_vm.at[s], dy_out.at[s], 2 + s).wait()
    put(dqkv_vm, dqkv_out, 6).start()
    for c in x_ring + dy_ring + [c for q in range(4) for c in far(q)]:
        c.wait_send()

    def others(c, _):
        at = pl.ds(pl.multiple_of(c * TILE, TILE), TILE)
        slots = (1, n - 1, 0)
        t = _dot(jnp.concatenate([dqkv_vm[s] for s in slots], axis=0), w_vm[at, :], 1, 1).astype(BF16)
        for m, s in enumerate(slots):
            dy_vm[s, :, at] = t[m * rows : (m + 1) * rows, :]
            count(t[m * rows : (m + 1) * rows, :], s, at)

    lax.fori_loop(0, deep // TILE, others, None)
    share = gain_s[...].sum(0, keepdims=True)
    for s in range(n):
        share_vm[s, :, :deep] = share
        share_vm[s, :, deep:] = dots_vm[s].T.sum(0, keepdims=True)
    shares_vm[me] = share_vm[0]
    shares = [send(share_vm.at[o], shares_vm.at[me], lax.rem(me + o, n), 33 + o) for o in range(1, n)]
    for c in shares + first(7):
        c.start()
    ends = [put(dy_vm.at[0], own_out, 7), put(dy_vm.at[1, high], right_b_out, 8), put(dy_vm.at[n - 1, low], left_a_out, 9), put(shares_vm, share_out, 10)]
    for c in ends[:3]:
        c.start()

    def sums(p):
        at = pl.ds(pl.multiple_of(p * eighth, eighth), eighth)
        return [put(in_vm.at[0, :, at], sum_a_out.at[:, at], 14 + 2 * p), put(in_vm.at[1, :, at], sum_b_out.at[:, at], 15 + 2 * p)]

    def add(p, _):
        at = pl.ds(pl.multiple_of(p * eighth, eighth), eighth)
        for c in first(p):
            c.wait_recv()
        in_vm[0, :, at] = (dy_vm[1, :half, at].astype(F32) + in_vm[0, :, at].astype(F32)).astype(BF16)
        in_vm[1, :, at] = (dy_vm[n - 1, half:, at].astype(F32) + in_vm[1, :, at].astype(F32)).astype(BF16)
        for c in sums(p):
            c.start()

    lax.fori_loop(0, 7, add, None)
    for c in shares:
        c.wait_recv()
    ends[3].start()
    add(7, None)
    for c in shares:
        c.wait_send()
    for p in range(8):
        for c in first(p):
            c.wait_send()
        ends += sums(p)
    for c in ends + [put(seen_vm, seen_out, 1), put(dqkv_vm, dqkv_out, 6)]:
        c.wait()


def gathered(n, x, dy, gain, wq, wk, wv, wo, table):
    rows, deep = x.shape
    width, d = wq.shape[1], wk.shape[1]
    g, half = width // d, rows // 2
    strips = g * rows // STRIP
    some = pl.BlockSpec(memory_space=pl.ANY)
    out = jax.ShapeDtypeStruct
    return pl.pallas_call(
        functools.partial(_kernel, n),
        in_specs=[some, some, pl.BlockSpec(memory_space=pltpu.VMEM)] + [some] * 5,
        out_specs=[some] * 10,
        out_shape=[out((n, 2, half, deep), BF16), out((n, rows, deep), BF16), out((n, rows, width), BF16), out((n, rows, width + 2 * d), BF16),
                   out((rows, deep), BF16)] + [out((half, deep), BF16)] * 4 + [out((n, 1, deep + rows), F32)],
        scratch_shapes=[
            pltpu.VMEM((n, rows, deep), BF16), pltpu.VMEM((deep, width + 2 * d), BF16),
            pltpu.VMEM((width, deep), BF16), pltpu.VMEM((n, rows, deep), BF16), pltpu.VMEM((n, rows, width), BF16),
            pltpu.VMEM((n, rows, width), BF16), pltpu.VMEM((rows, width), BF16), pltpu.VMEM((n, rows, width + 2 * d), BF16),
            pltpu.VMEM((n * rows, d), BF16), pltpu.VMEM((n * rows, d), BF16), pltpu.VMEM((n * rows, d), F32), pltpu.VMEM((n * rows, d), F32),
            pltpu.VMEM((n, strips, STRIP), F32), pltpu.VMEM((strips, STRIP), F32), pltpu.VMEM((strips, d + 8, STRIP), F32),
            pltpu.VMEM((strips, STRIP), F32), pltpu.VMEM((n * rows, d), F32), pltpu.VMEM((n * rows, d), F32),
            pltpu.VMEM((n, rows, 128), F32), pltpu.VMEM((2, half, deep), BF16), pltpu.VMEM((n, 1, deep + rows), F32), pltpu.VMEM((n, 1, deep + rows), F32),
            pltpu.VMEM((1, deep), F32), pltpu.VMEM((8, deep), F32), pltpu.VMEM((n, rows, 128), F32),
            pltpu.VMEM((2, strips, rows, STRIP), F32), pltpu.VMEM((rows, width), F32),
            pltpu.SemaphoreType.DMA((37,)), pltpu.SemaphoreType.DMA((37,)), pltpu.SemaphoreType.DMA((7,)), pltpu.SemaphoreType.DMA((30,)),
        ],
        compiler_params=pltpu.CompilerParams(collective_id=0, has_side_effects=True, vmem_limit_bytes=VMEM),
        cost_estimate=pl.CostEstimate(flops=60 * rows * deep * width, transcendentals=0, bytes_accessed=20 * rows * deep),
    )(x, dy, gain, wq, wk, wv, wo, table)


def _outer(a_ref, b_ref, *outs):
    t = _dot(a_ref[...], b_ref[...], 0, 0).astype(BF16)
    at = 0
    for o in outs:
        o[...] = t[:, at : at + o.shape[1]]
        at += o.shape[1]


def outer(a, b, widths):
    tokens, deep = a.shape
    tile = 2 * TILE
    return pl.pallas_call(
        _outer,
        grid=(deep // tile,),
        in_specs=[pl.BlockSpec((tokens, tile), lambda i: (0, i)), pl.BlockSpec(b.shape, lambda i: (0, 0))],
        out_specs=[pl.BlockSpec((tile, w), lambda i: (i, 0)) for w in widths],
        out_shape=[jax.ShapeDtypeStruct((deep, w), BF16) for w in widths],
        compiler_params=pltpu.CompilerParams(dimension_semantics=("arbitrary",), vmem_limit_bytes=24 * 2**20),
        cost_estimate=pl.CostEstimate(flops=2 * tokens * deep * b.shape[1], transcendentals=0, bytes_accessed=2 * deep * (tokens + b.shape[1])),
    )(a, b)


def solution(mesh):
    n = mesh.shape["tp"]

    def step(x, dy, gain, wq, wk, wv, wo):
        rows, deep = x.shape
        width = wq.shape[1]

        half_head = HEAD // 2
        rate = np.float32(THETA) ** (-np.arange(half_head, dtype=np.float32) / np.float32(half_head))
        angle = np.arange(n * rows, dtype=np.float32)[:, None] * rate
        table = jnp.asarray(np.concatenate([np.cos(angle), np.sin(angle)], 1))

        normal, dy_all, seen, dqkv, own, right_b, left_a, sum_a, sum_b, shares = gathered(n, x, dy, gain, wq, wk, wv, wo, table)

        def moved(t, places):
            return lax.ppermute(t, "tp", [(i, (i + places) % n) for i in range(n)])

        own_b, own_a = moved(right_b, 1), moved(left_a, -1)
        last_a, last_b = moved(sum_a, 1), moved(sum_b, -1)

        normal, dy_all, seen, dqkv = (t.reshape(n * rows, -1) for t in (normal, dy_all, seen, dqkv))
        by_wo = _dot(seen, dy_all, 0, 0).astype(BF16)
        by_wq, by_wk, by_wv = outer(normal, dqkv, (width, HEAD, HEAD))

        shares = shares.sum((0, 1))
        by_gain, mean = shares[None, :deep], shares[deep:, None] / deep

        wide, gain = x.astype(F32), gain.astype(F32)
        scale = lax.rsqrt(jnp.mean(wide * wide, -1, keepdims=True) + 1e-6)
        most = scale * ((own.astype(F32) + jnp.concatenate([own_a, own_b]).astype(F32)) * gain - wide * scale * mean) + dy.astype(F32)
        most = lax.optimization_barrier(most)
        by_x = most + scale * gain * jnp.concatenate([last_a, last_b]).astype(F32)
        return by_x.astype(BF16), by_gain, by_wq, by_wk, by_wv, by_wo

    tokens, columns = P(("dp", "tp"), None), P(None, "tp")
    return jax.shard_map(
        step,
        mesh=mesh,
        in_specs=(tokens, tokens, P(None), columns, columns, columns, P("tp", None)),
        out_specs=(tokens, P("dp", None), P("dp", "tp"), P("dp", "tp"), P("dp", "tp"), P(("dp", "tp"), None)),
        check_vma=False,
    )
```

```python
import functools

import jax
import jax.numpy as jnp
import numpy as np
from jax import lax
from jax.experimental import pallas as pl
from jax.experimental.pallas import tpu as pltpu
from jax.sharding import PartitionSpec as P

HEAD = 128
THETA = 10000
NEG = -1e30
HIDDEN = 2 * NEG
LOG2E = 1.4426950408889634
VMEM = 67043328
STRIP = 512
TILE = 256
F32, BF16 = jnp.float32, jnp.bfloat16


def _dot(a, b, ca, cb):
    return lax.dot_general(a, b, (((ca,), (cb,)), ((), ())), preferred_element_type=F32)


def _later(bk, cols, bq, first=0, jump=0):
    query = lax.rem(lax.broadcasted_iota(jnp.int32, (bk, cols), 1), bq)
    if jump:
        query += jnp.where(query >= bq // 2, jump, 0)
    return query + first >= lax.broadcasted_iota(jnp.int32, (bk, cols), 0)


def _kernel(n, x_ref, dy_ref, gain_ref, wq_ref, wk_ref, wv_ref, wo_ref, table_ref,
            a_out, dy_out, seen_out, dqkv_out, own_out, right_b_out, left_a_out, sum_a_out, sum_b_out, share_out,
            x_vm, w_vm, wo_vm, dy_vm, q_vm, seen_vm, ds_vm, dqkv_vm, k_vm, v_vm, dk_s, dv_s, lse_s, top_s, mix_s, delta_s,
            cos_vm, sin_vm, scale_s, in_vm, share_vm, shares_vm, gain_vm, gain_s, dots_vm, p_vm, acc_s, send_sem, recv_sem, load_sem, out_sem):
    rows, deep = x_ref.shape
    half = rows // 2
    d = k_vm.shape[1]
    dq_s, a_vm = mix_s.at[:, :d, :], in_vm
    width = wq_ref.shape[1]
    g = width // d
    per = STRIP // rows
    strips = g // per
    scale = d**-0.5
    e = scale * LOG2E
    me = lax.axis_index("tp")
    to_right, to_left = lax.rem(me + 1, n), lax.rem(me + n - 1, n)
    low, high = pl.ds(0, half), pl.ds(half, half)

    def start_of(s):
        return pl.multiple_of(lax.rem(me + s, n) * rows, rows)

    def send(src, dst, to, i):
        return pltpu.make_async_remote_copy(src_ref=src, dst_ref=dst, send_sem=send_sem.at[i], recv_sem=recv_sem.at[i],
                                            device_id={"tp": to}, device_id_type=pl.DeviceIdType.MESH)

    def load(src, dst, i):
        return pltpu.make_async_copy(src, dst, load_sem.at[i])

    def put(src, dst, i):
        return pltpu.make_async_copy(src, dst, out_sem.at[i])

    def ring(own, at, i):
        return [send(own.at[low], at.at[n - 1, low], to_right, i), send(own.at[high], at.at[1, high], to_left, i + 1),
                send(own.at[high], at.at[n - 1, high], to_right, i + 2), send(own.at[low], at.at[1, low], to_left, i + 3),
                send(at.at[n - 1, low], at.at[2, low], to_right, i + 4), send(at.at[1, high], at.at[2, high], to_left, i + 5)]

    quarter, eighth = deep // 4, deep // 8

    def far(r, q):
        at = pl.ds(pl.multiple_of(q * quarter, quarter), quarter)
        mine = [pl.ds(first + r * (half // 2), half // 2) for first in (0, half)]
        return [send(dy_vm.at[n - 1, mine[0], at], dy_vm.at[2, mine[0], at], to_right, 14 + 8 * r + 2 * q),
                send(dy_vm.at[1, mine[1], at], dy_vm.at[2, mine[1], at], to_left, 15 + 8 * r + 2 * q)]

    x_ring, dy_ring = ring(x_ref, x_vm, 0), ring(dy_ref, dy_vm, 6)[:4]
    loads = [load(x_ref, x_vm.at[0], 0), load(wq_ref, w_vm.at[:, pl.ds(0, width)], 1), load(wk_ref, w_vm.at[:, pl.ds(width, d)], 2),
             load(wv_ref, w_vm.at[:, pl.ds(width + d, d)], 3), load(table_ref, cos_vm, 4), load(dy_ref, dy_vm.at[0], 5), load(wo_ref, wo_vm, 6)]

    barrier = pltpu.get_barrier_semaphore()
    for o in range(1, n):
        pl.semaphore_signal(barrier, inc=1, device_id={"tp": lax.rem(me + o, n)}, device_id_type=pl.DeviceIdType.MESH)
    pl.semaphore_wait(barrier, n - 1)
    for c in x_ring[:4]:
        c.start()
    for c in loads:
        c.start()

    gain_vm[...] = gain_ref[...].astype(F32).reshape(1, deep)

    def turn(t, s, sign, at=0):
        here = pl.ds(pl.multiple_of(start_of(s) + at, half // 2), t.shape[0])
        return t * cos_vm[here, :] + sign * (pltpu.roll(t, d // 2, 1) * sin_vm[here, :])

    def project(i, _):
        s = i + i // 2 - 2 * (i // 3)

        @pl.when(i == 0)
        def _():
            for c in loads[:5]:
                c.wait()
            table = cos_vm[...]
            other = pltpu.roll(table, d // 2, 1)
            left_half = lax.broadcasted_iota(jnp.int32, table.shape, 1) < d // 2
            cos_vm[...] = jnp.where(left_half, table, other)
            sin_vm[...] = jnp.where(left_half, -other, table)

        @pl.when(i == 1)
        def _():
            for c in x_ring[:2]:
                c.wait_recv()
            for c in x_ring[4:] + dy_ring:
                c.start()
            for c in x_ring[2:4]:
                c.wait_recv()

        @pl.when(i == 3)
        def _():
            for c in x_ring[4:]:
                c.wait_recv()

        @pl.when(i > 0)
        def _():
            put(a_vm, a_out.at[0], 0).wait()

        def norm(r, _):
            some = pl.ds(pl.multiple_of(r * 16, 16), 16)
            t = x_vm[s, some, :].astype(F32)
            factor = lax.rsqrt(jnp.mean(t * t, -1, keepdims=True) + 1e-6)
            scale_s[s, some, :] = jnp.broadcast_to(factor, (16, 128))
            a_vm[r // (half // 16), pl.ds(pl.multiple_of(lax.rem(r * 16, half), 16), 16), :] = (t * factor * gain_vm[...]).astype(BF16)

        lax.fori_loop(0, rows // 16, norm, None)
        put(a_vm, a_out.at[s], 0).start()

        def tile(c, _):
            at = pl.multiple_of(c * TILE, TILE)
            t = _dot(a_vm[...].reshape(rows, deep), w_vm[:, pl.ds(at, TILE)], 1, 0).astype(BF16).astype(F32)
            for m in range(TILE // d):
                q_vm[s, :, pl.ds(pl.multiple_of(at + m * d, d), d)] = turn(t[:, m * d : (m + 1) * d], s, 1).astype(BF16)

        lax.fori_loop(0, width // TILE, tile, None)
        t = _dot(a_vm[...].reshape(rows, deep), w_vm[:, width:], 1, 0).astype(BF16)
        k_vm[pl.ds(start_of(s), rows), :] = turn(t[:, :d].astype(F32), s, 1).astype(BF16)
        v_vm[pl.ds(start_of(s), rows), :] = t[:, d:]

    lax.fori_loop(0, n, project, None)

    def heads(ref, first):
        return jnp.concatenate([ref[:, h * d : (h + 1) * d] for h in range(first, first + per)], axis=0)

    ones = jnp.ones((8, rows), BF16)

    def forward(s, _):
        top_s[...] = jnp.full_like(top_s, NEG)
        mix_s[...] = jnp.zeros_like(mix_s)

        def block(j, masked):
            here = pl.ds(pl.multiple_of(j * rows, rows), rows)
            keys = k_vm[here, :]
            values = jnp.concatenate([v_vm[here, :].T, ones], axis=0)
            scores = [_dot(keys, heads(q_vm.at[s], c * per), 1, 1) for c in range(strips)]
            weights, keeps = [], []
            for c, t in enumerate(scores):
                if masked:
                    t = jnp.where(_later(rows, STRIP, rows), t, HIDDEN)
                old = top_s[c : c + 1, :]
                top = jnp.maximum(old, t.max(axis=0, keepdims=True))
                top_s[c : c + 1, :] = top
                weights.append(jnp.exp2((t - top) * e).astype(BF16))
                keeps.append(jnp.exp2((old - top) * e))
            for c in range(strips):
                mix_s[c] = mix_s[c] * keeps[c] + _dot(values, weights[c], 1, 0)

        whole = lax.rem(me + s, n)
        lax.fori_loop(0, whole, lambda j, _: block(j, False), None)
        block(whole, True)
        for c in range(strips):
            total = mix_s[c, d : d + 1, :]
            out = (mix_s[c, :d, :] * (1 / total)).T
            lse_s[s, c : c + 1, :] = top_s[c : c + 1, :] * e + jnp.log(total) * LOG2E
            for m in range(per):
                h = c * per + m
                seen_vm[s, :, h * d : (h + 1) * d] = out[m * rows : (m + 1) * rows, :].astype(BF16)

    lax.fori_loop(0, n, forward, None)
    put(seen_vm, seen_out, 1).start()

    dk_s[...] = jnp.zeros_like(dk_s)
    dv_s[...] = jnp.zeros_like(dv_s)

    each = STRIP // half

    def pieces(at, r):
        return [pl.ds(at, half)] if at is not None else [pl.ds(first + r * (half // 2), half // 2) for first in (0, half)]

    def parts(ref, there):
        return [jnp.concatenate([ref[k, h * d : (h + 1) * d] for h in range(c, c + each) for k in there], axis=0) for c in range(0, g, each)]

    def delta(s, at, r, mine):
        for h in range(g):
            cols = slice(h * d, (h + 1) * d)
            seen = jnp.concatenate([seen_vm[s, k, cols] for k in pieces(at, r)], axis=0)
            both = ds_vm[mine, cols].astype(F32) * seen.astype(F32)
            c, m = divmod(h, each)
            delta_s[c : c + 1, m * half : (m + 1) * half] = both.T.sum(axis=0, keepdims=True)

    def lse_of(s, at, r, h):
        k, m = divmod(h, per)
        if at is not None:
            return lse_s[s, k : k + 1, pl.ds(pl.multiple_of(m * rows + at, half), half)]
        low, high = (lse_s[s, k : k + 1, m * rows + first : m * rows + first + half] for first in (0, half))
        first = lax.broadcasted_iota(jnp.int32, low.shape, 1) < half // 2
        return jnp.where(first, low, pltpu.roll(high, half // 2, 1)) if r == 0 else jnp.where(first, pltpu.roll(low, half // 2, 1), high)

    def weigh(s, at, r, c, scores, masked):
        p = jnp.exp2(scores * e - jnp.concatenate([lse_of(s, at, r, h) for h in range(c * each, (c + 1) * each)], axis=1))
        if not masked:
            return p
        return jnp.where(_later(rows, STRIP, half, at) if at is not None else _later(rows, STRIP, half, r * (half // 2), half // 2), p, 0.0)

    def fresh(s, at, r, masked):
        def weights(keys, qs):
            scores = [_dot(keys, t, 1, 1) for t in qs]
            return lambda c: weigh(s, at, r, c, scores[c], masked)
        return weights

    def back(s, at, r, mine, j, weights):
        here = pl.ds(pl.multiple_of(j * rows, rows), rows)
        keys, values = k_vm[here, :], v_vm[here, :]
        qs, dos = parts(q_vm.at[s], pieces(at, r)), parts(ds_vm, [mine])
        ps = weights(keys, qs)
        dps = [_dot(values, t, 1, 1) for t in dos]
        for c in range(len(qs)):
            p = ps(c)
            ds = (p * (dps[c] - delta_s[c : c + 1, :])).astype(BF16)
            dv_s[here, :] += _dot(p.astype(BF16), dos[c], 1, 0)
            dk_s[here, :] += _dot(ds, qs[c], 1, 0)
            dq_s[c] += _dot(keys.T, ds, 1, 0)

    def dq_out(s, at, r):
        for h in range(g):
            c, m = divmod(h, each)
            dq = (dq_s[c, :, m * half : (m + 1) * half] * scale).T
            some = pieces(at, r)
            long = half // len(some)
            for k, there in enumerate(some):
                dqkv_vm[s, there, h * d : (h + 1) * d] = turn(dq[k * long : (k + 1) * long, :], s, -1, there.start).astype(BF16)

    opposite_place = lax.rem(me + 2, n)

    def ahead(j, masked):
        keys = k_vm[pl.ds(pl.multiple_of(j * rows, rows), rows), :]
        for c, t in enumerate(parts(q_vm.at[2], pieces(None, 1))):
            p_vm[j, c] = weigh(2, None, 1, c, _dot(keys, t, 1, 1), masked)

    def near(i, _):
        pair, second = i // 2, lax.rem(i, 2)
        s = ((pair + 1) // 2) * (n - 1 - 2 * second)
        at = pl.multiple_of(half * lax.rem(second + pair // 2, 2), half)

        @pl.when(i == 0)
        def _():
            for c in loads[5:]:
                c.wait()
            put(dy_vm.at[0], dy_out.at[0], 2).start()

        @pl.when(i == 2)
        def _():
            put(a_vm, a_out.at[0], 0).wait()
            for c in dy_ring[:2]:
                c.wait_recv()
            for r in range(2):
                for q in range(4):
                    for c in far(r, q):
                        c.start()

        @pl.when(i == 4)
        def _():
            lax.fori_loop(0, opposite_place, lambda j, _: ahead(j, False), None)
            ahead(opposite_place, True)
            for c in dy_ring[2:]:
                c.wait_recv()
            for k in (1, n - 1):
                put(dy_vm.at[k], dy_out.at[k], 2 + k).start()

        @pl.when(second == 0)
        def _():
            other = (pair + 1) // 2
            there = pl.ds(pl.multiple_of(half - at, half), half)

            def tile(c, _):
                cols = pl.ds(pl.multiple_of(c * TILE, TILE), TILE)
                both = jnp.concatenate([dy_vm[s, pl.ds(at, half), :], dy_vm[other, there, :]], axis=0)
                ds_vm[:, cols] = _dot(both, wo_vm[cols, :], 1, 1).astype(BF16)

            lax.fori_loop(0, width // TILE, tile, None)

        mine = pl.ds(pl.multiple_of(second * half, half), half)
        dq_s[...] = jnp.zeros_like(dq_s)
        delta(s, at, None, mine)
        whole = lax.rem(me + s, n)
        lax.fori_loop(0, whole, lambda j, _: back(s, at, None, mine, j, fresh(s, at, None, False)), None)
        back(s, at, None, mine, whole, fresh(s, at, None, True))
        dq_out(s, at, None)

    lax.fori_loop(0, 6, near, None)

    gain_s[...] = jnp.zeros_like(gain_s)
    dots_vm[...] = jnp.zeros_like(dots_vm)
    for r in range(2):
        mine = pl.ds(r * half, half)
        dq_s[...] = jnp.zeros_like(dq_s)
        acc_s[...] = jnp.zeros_like(acc_s)

        def through(q, _):
            for c in far(r, q):
                c.wait_recv()
            part = pl.ds(pl.multiple_of(q * quarter, quarter), quarter)

            def tile(c, _):
                cols = pl.ds(pl.multiple_of(c * TILE, TILE), TILE)
                both = jnp.concatenate([dy_vm[2, k, part] for k in pieces(None, r)], axis=0)
                acc_s[:, cols] += _dot(both, wo_vm[cols, part], 1, 1)

            lax.fori_loop(0, width // TILE, tile, None)

        lax.fori_loop(0, 4, through, None)
        if r == 1:
            put(dy_vm.at[2], dy_out.at[2], 4).start()
        ds_vm[mine, :] = acc_s[...].astype(BF16)
        delta(2, None, r, mine)
        if r == 0:
            lax.fori_loop(0, opposite_place, lambda j, _: back(2, None, r, mine, j, fresh(2, None, r, False)), None)
            back(2, None, r, mine, opposite_place, fresh(2, None, r, True))
        else:
            lax.fori_loop(0, opposite_place + 1, lambda j, _: back(2, None, r, mine, j, lambda keys, qs: lambda c: p_vm[j, c]), None)
        dq_out(2, None, r)

    def dkv_out(s):
        here = pl.ds(start_of(s), rows)
        dqkv_vm[s, :, width : width + d] = turn(dk_s[here, :] * scale, s, -1).astype(BF16)
        dqkv_vm[s, :, width + d :] = dv_s[here, :].astype(BF16)

    dkv_out(2)
    put(dy_vm.at[2], dy_out.at[2], 4).wait()

    def first(p):
        at = pl.ds(pl.multiple_of(p * eighth, eighth), eighth)
        return [send(dy_vm.at[2, low, at], in_vm.at[0, :, at], to_right, 30 + 2 * p), send(dy_vm.at[2, high, at], in_vm.at[1, :, at], to_left, 31 + 2 * p)]

    def count(t, s, at):
        unit = x_vm[s, :, at].astype(F32) * jnp.concatenate([scale_s[s]] * (t.shape[1] // 128), axis=1)
        both = t.astype(F32) * unit
        gain_s[:, at] += both.reshape(rows // 8, 8, t.shape[1]).sum(0)
        both = both * gain_vm[:, at]
        dots_vm[s] += sum(both[:, m : m + 128] for m in range(0, t.shape[1], 128))

    def opposite(c, _):
        at = pl.ds(pl.multiple_of(c * eighth, eighth), eighth)
        t = _dot(dqkv_vm[2], w_vm[at, :], 1, 1).astype(BF16)
        dy_vm[2, :, at] = t

        @pl.when(c < 7)
        def _():
            for k in first(c):
                k.start()

        count(t, 2, at)

    lax.fori_loop(0, 8, opposite, None)
    for s in (0, 1, n - 1):
        dkv_out(s)
        put(dy_vm.at[s], dy_out.at[s], 2 + s).wait()
    put(dqkv_vm, dqkv_out, 6).start()
    for c in x_ring + dy_ring + [c for r in range(2) for q in range(4) for c in far(r, q)]:
        c.wait_send()

    def others(c, _):
        at = pl.ds(pl.multiple_of(c * TILE, TILE), TILE)
        slots = (1, n - 1, 0)
        t = _dot(jnp.concatenate([dqkv_vm[s] for s in slots], axis=0), w_vm[at, :], 1, 1).astype(BF16)
        for m, s in enumerate(slots):
            dy_vm[s, :, at] = t[m * rows : (m + 1) * rows, :]
            count(t[m * rows : (m + 1) * rows, :], s, at)

    lax.fori_loop(0, deep // TILE, others, None)
    share = gain_s[...].sum(0, keepdims=True)
    for s in range(n):
        share_vm[s, :, :deep] = share
        share_vm[s, :, deep:] = dots_vm[s].T.sum(0, keepdims=True)
    shares_vm[me] = share_vm[0]
    shares = [send(share_vm.at[o], shares_vm.at[me], lax.rem(me + o, n), 45 + o) for o in range(1, n)]
    for c in shares + first(7):
        c.start()
    ends = [put(dy_vm.at[0], own_out, 7), put(dy_vm.at[1, high], right_b_out, 8), put(dy_vm.at[n - 1, low], left_a_out, 9), put(shares_vm, share_out, 10)]
    for c in ends[:3]:
        c.start()

    def sums(p):
        at = pl.ds(pl.multiple_of(p * eighth, eighth), eighth)
        return [put(in_vm.at[0, :, at], sum_a_out.at[:, at], 14 + 2 * p), put(in_vm.at[1, :, at], sum_b_out.at[:, at], 15 + 2 * p)]

    def add(p, _):
        at = pl.ds(pl.multiple_of(p * eighth, eighth), eighth)
        for c in first(p):
            c.wait_recv()
        in_vm[0, :, at] = (dy_vm[1, :half, at].astype(F32) + in_vm[0, :, at].astype(F32)).astype(BF16)
        in_vm[1, :, at] = (dy_vm[n - 1, half:, at].astype(F32) + in_vm[1, :, at].astype(F32)).astype(BF16)
        for c in sums(p):
            c.start()

    lax.fori_loop(0, 7, add, None)
    for c in shares:
        c.wait_recv()
    ends[3].start()
    add(7, None)
    for c in shares:
        c.wait_send()
    for p in range(8):
        for c in first(p):
            c.wait_send()
        ends += sums(p)
    for c in ends + [put(seen_vm, seen_out, 1), put(dqkv_vm, dqkv_out, 6)]:
        c.wait()


def gathered(n, x, dy, gain, wq, wk, wv, wo, table):
    rows, deep = x.shape
    width, d = wq.shape[1], wk.shape[1]
    g, half = width // d, rows // 2
    strips = g * rows // STRIP
    some = pl.BlockSpec(memory_space=pl.ANY)
    out = jax.ShapeDtypeStruct
    return pl.pallas_call(
        functools.partial(_kernel, n),
        in_specs=[some, some, pl.BlockSpec(memory_space=pltpu.VMEM)] + [some] * 5,
        out_specs=[some] * 10,
        out_shape=[out((n, 2, half, deep), BF16), out((n, rows, deep), BF16), out((n, rows, width), BF16), out((n, rows, width + 2 * d), BF16),
                   out((rows, deep), BF16)] + [out((half, deep), BF16)] * 4 + [out((n, 1, deep + rows), F32)],
        scratch_shapes=[
            pltpu.VMEM((n, rows, deep), BF16), pltpu.VMEM((deep, width + 2 * d), BF16),
            pltpu.VMEM((width, deep), BF16), pltpu.VMEM((n, rows, deep), BF16), pltpu.VMEM((n, rows, width), BF16),
            pltpu.VMEM((n, rows, width), BF16), pltpu.VMEM((rows, width), BF16), pltpu.VMEM((n, rows, width + 2 * d), BF16),
            pltpu.VMEM((n * rows, d), BF16), pltpu.VMEM((n * rows, d), BF16), pltpu.VMEM((n * rows, d), F32), pltpu.VMEM((n * rows, d), F32),
            pltpu.VMEM((n, strips, STRIP), F32), pltpu.VMEM((strips, STRIP), F32), pltpu.VMEM((strips, d + 8, STRIP), F32),
            pltpu.VMEM((strips, STRIP), F32), pltpu.VMEM((n * rows, d), F32), pltpu.VMEM((n * rows, d), F32),
            pltpu.VMEM((n, rows, 128), F32), pltpu.VMEM((2, half, deep), BF16), pltpu.VMEM((n, 1, deep + rows), F32), pltpu.VMEM((n, 1, deep + rows), F32),
            pltpu.VMEM((1, deep), F32), pltpu.VMEM((8, deep), F32), pltpu.VMEM((n, rows, 128), F32),
            pltpu.VMEM((n, strips // 2, rows, STRIP), F32), pltpu.VMEM((half, width), F32),
            pltpu.SemaphoreType.DMA((49,)), pltpu.SemaphoreType.DMA((49,)), pltpu.SemaphoreType.DMA((7,)), pltpu.SemaphoreType.DMA((30,)),
        ],
        compiler_params=pltpu.CompilerParams(collective_id=0, has_side_effects=True, vmem_limit_bytes=VMEM),
        cost_estimate=pl.CostEstimate(flops=60 * rows * deep * width, transcendentals=0, bytes_accessed=20 * rows * deep),
    )(x, dy, gain, wq, wk, wv, wo, table)


def _outer(a_ref, b_ref, *outs):
    t = _dot(a_ref[...], b_ref[...], 0, 0).astype(BF16)
    at = 0
    for o in outs:
        o[...] = t[:, at : at + o.shape[1]]
        at += o.shape[1]


def outer(a, b, widths):
    tokens, deep = a.shape
    tile = 2 * TILE
    return pl.pallas_call(
        _outer,
        grid=(deep // tile,),
        in_specs=[pl.BlockSpec((tokens, tile), lambda i: (0, i)), pl.BlockSpec(b.shape, lambda i: (0, 0))],
        out_specs=[pl.BlockSpec((tile, w), lambda i: (i, 0)) for w in widths],
        out_shape=[jax.ShapeDtypeStruct((deep, w), BF16) for w in widths],
        compiler_params=pltpu.CompilerParams(dimension_semantics=("arbitrary",), vmem_limit_bytes=24 * 2**20),
        cost_estimate=pl.CostEstimate(flops=2 * tokens * deep * b.shape[1], transcendentals=0, bytes_accessed=2 * deep * (tokens + b.shape[1])),
    )(a, b)


def solution(mesh):
    n = mesh.shape["tp"]

    def step(x, dy, gain, wq, wk, wv, wo):
        rows, deep = x.shape
        width = wq.shape[1]

        half_head = HEAD // 2
        rate = np.float32(THETA) ** (-np.arange(half_head, dtype=np.float32) / np.float32(half_head))
        angle = np.arange(n * rows, dtype=np.float32)[:, None] * rate
        table = jnp.asarray(np.concatenate([np.cos(angle), np.sin(angle)], 1))

        normal, dy_all, seen, dqkv, own, right_b, left_a, sum_a, sum_b, shares = gathered(n, x, dy, gain, wq, wk, wv, wo, table)

        def moved(t, places):
            return lax.ppermute(t, "tp", [(i, (i + places) % n) for i in range(n)])

        own_b, own_a = moved(right_b, 1), moved(left_a, -1)
        last_a, last_b = moved(sum_a, 1), moved(sum_b, -1)

        normal, dy_all, seen, dqkv = (t.reshape(n * rows, -1) for t in (normal, dy_all, seen, dqkv))
        by_wo = _dot(seen, dy_all, 0, 0).astype(BF16)
        by_wq, by_wk, by_wv = outer(normal, dqkv, (width, HEAD, HEAD))

        shares = shares.sum((0, 1))
        by_gain, mean = shares[None, :deep], shares[deep:, None] / deep

        wide, gain = x.astype(F32), gain.astype(F32)
        scale = lax.rsqrt(jnp.mean(wide * wide, -1, keepdims=True) + 1e-6)
        most = scale * ((own.astype(F32) + jnp.concatenate([own_a, own_b]).astype(F32)) * gain - wide * scale * mean) + dy.astype(F32)
        most = lax.optimization_barrier(most)
        by_x = most + scale * gain * jnp.concatenate([last_a, last_b]).astype(F32)
        return by_x.astype(BF16), by_gain, by_wq, by_wk, by_wv, by_wo

    tokens, columns = P(("dp", "tp"), None), P(None, "tp")
    return jax.shard_map(
        step,
        mesh=mesh,
        in_specs=(tokens, tokens, P(None), columns, columns, columns, P("tp", None)),
        out_specs=(tokens, P("dp", None), P("dp", "tp"), P("dp", "tp"), P("dp", "tp"), P(("dp", "tp"), None)),
        check_vma=False,
    )
```

```python
import functools

import jax
import jax.numpy as jnp
import numpy as np
from jax import lax
from jax.experimental import pallas as pl
from jax.experimental.pallas import tpu as pltpu
from jax.sharding import PartitionSpec as P

HEAD = 128
THETA = 10000
NEG = -1e30
HIDDEN = 2 * NEG
LOG2E = 1.4426950408889634
VMEM = 67043328
STRIP = 512
TILE = 256
F32, BF16 = jnp.float32, jnp.bfloat16


def _dot(a, b, ca, cb):
    return lax.dot_general(a, b, (((ca,), (cb,)), ((), ())), preferred_element_type=F32)


def _later(bk, cols, bq, first=0, jump=0):
    query = lax.rem(lax.broadcasted_iota(jnp.int32, (bk, cols), 1), bq)
    if jump:
        query += jnp.where(query >= bq // 2, jump, 0)
    return query + first >= lax.broadcasted_iota(jnp.int32, (bk, cols), 0)


def _kernel(n, x_ref, dy_ref, gain_ref, wq_ref, wk_ref, wv_ref, wo_ref, table_ref,
            a_out, dy_out, seen_out, dqkv_out, own_out, right_b_out, left_a_out, sum_a_out, sum_b_out, share_out,
            x_vm, w_vm, wo_vm, dy_vm, q_vm, seen_vm, ds_vm, dqkv_vm, k_vm, v_vm, dk_s, dv_s, lse_s, top_s, mix_s, delta_s,
            cos_vm, sin_vm, scale_s, in_vm, share_vm, shares_vm, gain_vm, gain_s, dots_vm, p_vm, acc_s, send_sem, recv_sem, load_sem, out_sem):
    rows, deep = x_ref.shape
    half = rows // 2
    d = k_vm.shape[1]
    dq_s, a_vm = mix_s.at[:, :d, :], in_vm
    width = wq_ref.shape[1]
    g = width // d
    per = STRIP // rows
    strips = g // per
    scale = d**-0.5
    e = scale * LOG2E
    me = lax.axis_index("tp")
    to_right, to_left = lax.rem(me + 1, n), lax.rem(me + n - 1, n)
    low, high = pl.ds(0, half), pl.ds(half, half)

    def start_of(s):
        return pl.multiple_of(lax.rem(me + s, n) * rows, rows)

    def send(src, dst, to, i):
        return pltpu.make_async_remote_copy(src_ref=src, dst_ref=dst, send_sem=send_sem.at[i], recv_sem=recv_sem.at[i],
                                            device_id={"tp": to}, device_id_type=pl.DeviceIdType.MESH)

    def load(src, dst, i):
        return pltpu.make_async_copy(src, dst, load_sem.at[i])

    def put(src, dst, i):
        return pltpu.make_async_copy(src, dst, out_sem.at[i])

    def ring(own, at, i):
        return [send(own.at[low], at.at[n - 1, low], to_right, i), send(own.at[high], at.at[1, high], to_left, i + 1),
                send(own.at[high], at.at[n - 1, high], to_right, i + 2), send(own.at[low], at.at[1, low], to_left, i + 3),
                send(at.at[n - 1, low], at.at[2, low], to_right, i + 4), send(at.at[1, high], at.at[2, high], to_left, i + 5)]

    quarter, eighth = deep // 4, deep // 8

    def far(r, q):
        at = pl.ds(pl.multiple_of(q * quarter, quarter), quarter)
        mine = [pl.ds(first + r * (half // 2), half // 2) for first in (0, half)]
        return [send(dy_vm.at[n - 1, mine[0], at], dy_vm.at[2, mine[0], at], to_right, 14 + 8 * r + 2 * q),
                send(dy_vm.at[1, mine[1], at], dy_vm.at[2, mine[1], at], to_left, 15 + 8 * r + 2 * q)]

    x_ring, dy_ring = ring(x_ref, x_vm, 0), ring(dy_ref, dy_vm, 6)[:4]
    loads = [load(x_ref, x_vm.at[0], 0), load(wq_ref, w_vm.at[:, pl.ds(0, width)], 1), load(wk_ref, w_vm.at[:, pl.ds(width, d)], 2),
             load(wv_ref, w_vm.at[:, pl.ds(width + d, d)], 3), load(table_ref, cos_vm, 4), load(dy_ref, dy_vm.at[0], 5), load(wo_ref, wo_vm, 6)]

    barrier = pltpu.get_barrier_semaphore()
    for neighbour in (to_right, to_left):
        pl.semaphore_signal(barrier, inc=1, device_id={"tp": neighbour}, device_id_type=pl.DeviceIdType.MESH)
    pl.semaphore_wait(barrier, 2)
    for c in x_ring[:4]:
        c.start()
    for c in loads:
        c.start()

    gain_vm[...] = gain_ref[...].astype(F32).reshape(1, deep)

    def turn(t, s, sign, at=0):
        here = pl.ds(pl.multiple_of(start_of(s) + at, half // 2), t.shape[0])
        return t * cos_vm[here, :] + sign * (pltpu.roll(t, d // 2, 1) * sin_vm[here, :])

    def project(i, _):
        s = i + i // 2 - 2 * (i // 3)

        @pl.when(i == 0)
        def _():
            for c in loads[:5]:
                c.wait()
            table = cos_vm[...]
            other = pltpu.roll(table, d // 2, 1)
            left_half = lax.broadcasted_iota(jnp.int32, table.shape, 1) < d // 2
            cos_vm[...] = jnp.where(left_half, table, other)
            sin_vm[...] = jnp.where(left_half, -other, table)

        @pl.when(i == 1)
        def _():
            for c in x_ring[:2]:
                c.wait_recv()
            for c in x_ring[4:] + dy_ring:
                c.start()
            for c in x_ring[2:4]:
                c.wait_recv()

        @pl.when(i == 3)
        def _():
            for c in x_ring[4:]:
                c.wait_recv()

        @pl.when(i > 0)
        def _():
            put(a_vm, a_out.at[0], 0).wait()

        def norm(r, _):
            some = pl.ds(pl.multiple_of(r * 16, 16), 16)
            t = x_vm[s, some, :].astype(F32)
            factor = lax.rsqrt(jnp.mean(t * t, -1, keepdims=True) + 1e-6)
            scale_s[s, some, :] = jnp.broadcast_to(factor, (16, 128))
            a_vm[r // (half // 16), pl.ds(pl.multiple_of(lax.rem(r * 16, half), 16), 16), :] = (t * factor * gain_vm[...]).astype(BF16)

        lax.fori_loop(0, rows // 16, norm, None)
        put(a_vm, a_out.at[s], 0).start()

        def tile(c, _):
            at = pl.multiple_of(c * TILE, TILE)
            t = _dot(a_vm[...].reshape(rows, deep), w_vm[:, pl.ds(at, TILE)], 1, 0).astype(BF16).astype(F32)
            for m in range(TILE // d):
                q_vm[s, :, pl.ds(pl.multiple_of(at + m * d, d), d)] = turn(t[:, m * d : (m + 1) * d], s, 1).astype(BF16)

        lax.fori_loop(0, width // TILE, tile, None)
        t = _dot(a_vm[...].reshape(rows, deep), w_vm[:, width:], 1, 0).astype(BF16)
        k_vm[pl.ds(start_of(s), rows), :] = turn(t[:, :d].astype(F32), s, 1).astype(BF16)
        v_vm[pl.ds(start_of(s), rows), :] = t[:, d:]

    lax.fori_loop(0, n, project, None)

    def heads(ref, first):
        return jnp.concatenate([ref[:, h * d : (h + 1) * d] for h in range(first, first + per)], axis=0)

    ones = jnp.ones((8, rows), BF16)

    def forward(s, _):
        top_s[...] = jnp.full_like(top_s, NEG)
        mix_s[...] = jnp.zeros_like(mix_s)

        def block(j, masked):
            here = pl.ds(pl.multiple_of(j * rows, rows), rows)
            keys = k_vm[here, :]
            values = jnp.concatenate([v_vm[here, :].T, ones], axis=0)
            scores = [_dot(keys, heads(q_vm.at[s], c * per), 1, 1) for c in range(strips)]
            weights, keeps = [], []
            for c, t in enumerate(scores):
                if masked:
                    t = jnp.where(_later(rows, STRIP, rows), t, HIDDEN)
                old = top_s[c : c + 1, :]
                top = jnp.maximum(old, t.max(axis=0, keepdims=True))
                top_s[c : c + 1, :] = top
                weights.append(jnp.exp2((t - top) * e).astype(BF16))
                keeps.append(jnp.exp2((old - top) * e))
            for c in range(strips):
                mix_s[c] = mix_s[c] * keeps[c] + _dot(values, weights[c], 1, 0)

        whole = lax.rem(me + s, n)
        lax.fori_loop(0, whole, lambda j, _: block(j, False), None)
        block(whole, True)
        for c in range(strips):
            total = mix_s[c, d : d + 1, :]
            out = (mix_s[c, :d, :] * (1 / total)).T
            lse_s[s, c : c + 1, :] = top_s[c : c + 1, :] * e + jnp.log(total) * LOG2E
            for m in range(per):
                h = c * per + m
                seen_vm[s, :, h * d : (h + 1) * d] = out[m * rows : (m + 1) * rows, :].astype(BF16)

    lax.fori_loop(0, n, forward, None)
    put(seen_vm, seen_out, 1).start()

    dk_s[...] = jnp.zeros_like(dk_s)
    dv_s[...] = jnp.zeros_like(dv_s)

    each = STRIP // half

    def pieces(at, r):
        return [pl.ds(at, half)] if at is not None else [pl.ds(first + r * (half // 2), half // 2) for first in (0, half)]

    def parts(ref, there):
        return [jnp.concatenate([ref[k, h * d : (h + 1) * d] for h in range(c, c + each) for k in there], axis=0) for c in range(0, g, each)]

    def delta(s, at, r, mine):
        for h in range(g):
            cols = slice(h * d, (h + 1) * d)
            seen = jnp.concatenate([seen_vm[s, k, cols] for k in pieces(at, r)], axis=0)
            both = ds_vm[mine, cols].astype(F32) * seen.astype(F32)
            c, m = divmod(h, each)
            delta_s[c : c + 1, m * half : (m + 1) * half] = both.T.sum(axis=0, keepdims=True)

    def lse_of(s, at, r, h):
        k, m = divmod(h, per)
        if at is not None:
            return lse_s[s, k : k + 1, pl.ds(pl.multiple_of(m * rows + at, half), half)]
        low, high = (lse_s[s, k : k + 1, m * rows + first : m * rows + first + half] for first in (0, half))
        first = lax.broadcasted_iota(jnp.int32, low.shape, 1) < half // 2
        return jnp.where(first, low, pltpu.roll(high, half // 2, 1)) if r == 0 else jnp.where(first, pltpu.roll(low, half // 2, 1), high)

    def weigh(s, at, r, c, scores, masked):
        p = jnp.exp2(scores * e - jnp.concatenate([lse_of(s, at, r, h) for h in range(c * each, (c + 1) * each)], axis=1))
        if not masked:
            return p
        return jnp.where(_later(rows, STRIP, half, at) if at is not None else _later(rows, STRIP, half, r * (half // 2), half // 2), p, 0.0)

    def fresh(s, at, r, masked):
        def weights(keys, qs):
            scores = [_dot(keys, t, 1, 1) for t in qs]
            return lambda c: weigh(s, at, r, c, scores[c], masked)
        return weights

    def back(s, at, r, mine, j, weights):
        here = pl.ds(pl.multiple_of(j * rows, rows), rows)
        keys, values = k_vm[here, :], v_vm[here, :]
        qs, dos = parts(q_vm.at[s], pieces(at, r)), parts(ds_vm, [mine])
        ps = weights(keys, qs)
        dps = [_dot(values, t, 1, 1) for t in dos]
        for c in range(len(qs)):
            p = ps(c)
            ds = (p * (dps[c] - delta_s[c : c + 1, :])).astype(BF16)
            dv_s[here, :] += _dot(p.astype(BF16), dos[c], 1, 0)
            dk_s[here, :] += _dot(ds, qs[c], 1, 0)
            dq_s[c] += _dot(keys.T, ds, 1, 0)

    def dq_out(s, at, r):
        for h in range(g):
            c, m = divmod(h, each)
            dq = (dq_s[c, :, m * half : (m + 1) * half] * scale).T
            some = pieces(at, r)
            long = half // len(some)
            for k, there in enumerate(some):
                dqkv_vm[s, there, h * d : (h + 1) * d] = turn(dq[k * long : (k + 1) * long, :], s, -1, there.start).astype(BF16)

    opposite_place = lax.rem(me + 2, n)

    def ahead(j, masked):
        keys = k_vm[pl.ds(pl.multiple_of(j * rows, rows), rows), :]
        for c, t in enumerate(parts(q_vm.at[2], pieces(None, 1))):
            p_vm[j, c] = weigh(2, None, 1, c, _dot(keys, t, 1, 1), masked)

    def near(i, _):
        pair, second = i // 2, lax.rem(i, 2)
        s = ((pair + 1) // 2) * (n - 1 - 2 * second)
        at = pl.multiple_of(half * lax.rem(second + pair // 2, 2), half)

        @pl.when(i == 0)
        def _():
            for c in loads[5:]:
                c.wait()
            put(dy_vm.at[0], dy_out.at[0], 2).start()

        @pl.when(i == 2)
        def _():
            put(a_vm, a_out.at[0], 0).wait()
            for c in dy_ring[:2]:
                c.wait_recv()
            for r in range(2):
                for q in range(4):
                    for c in far(r, q):
                        c.start()

        @pl.when(i == 4)
        def _():
            lax.fori_loop(0, opposite_place, lambda j, _: ahead(j, False), None)
            ahead(opposite_place, True)
            for c in dy_ring[2:]:
                c.wait_recv()
            for k in (1, n - 1):
                put(dy_vm.at[k], dy_out.at[k], 2 + k).start()

        @pl.when(second == 0)
        def _():
            other = (pair + 1) // 2
            there = pl.ds(pl.multiple_of(half - at, half), half)

            def tile(c, _):
                cols = pl.ds(pl.multiple_of(c * TILE, TILE), TILE)
                both = jnp.concatenate([dy_vm[s, pl.ds(at, half), :], dy_vm[other, there, :]], axis=0)
                ds_vm[:, cols] = _dot(both, wo_vm[cols, :], 1, 1).astype(BF16)

            lax.fori_loop(0, width // TILE, tile, None)

        mine = pl.ds(pl.multiple_of(second * half, half), half)
        dq_s[...] = jnp.zeros_like(dq_s)
        delta(s, at, None, mine)
        whole = lax.rem(me + s, n)
        lax.fori_loop(0, whole, lambda j, _: back(s, at, None, mine, j, fresh(s, at, None, False)), None)
        back(s, at, None, mine, whole, fresh(s, at, None, True))
        dq_out(s, at, None)

    lax.fori_loop(0, 6, near, None)

    gain_s[...] = jnp.zeros_like(gain_s)
    dots_vm[...] = jnp.zeros_like(dots_vm)
    for r in range(2):
        mine = pl.ds(r * half, half)
        dq_s[...] = jnp.zeros_like(dq_s)
        acc_s[...] = jnp.zeros_like(acc_s)

        def through(q, _):
            for c in far(r, q):
                c.wait_recv()
            part = pl.ds(pl.multiple_of(q * quarter, quarter), quarter)

            both = jnp.concatenate([dy_vm[2, k, part] for k in pieces(None, r)], axis=0)
            acc_s[...] += _dot(both, wo_vm[:, part], 1, 1)

        lax.fori_loop(0, 4, through, None)
        if r == 1:
            put(dy_vm.at[2], dy_out.at[2], 4).start()
        ds_vm[mine, :] = acc_s[...].astype(BF16)
        delta(2, None, r, mine)
        if r == 0:
            lax.fori_loop(0, opposite_place, lambda j, _: back(2, None, r, mine, j, fresh(2, None, r, False)), None)
            back(2, None, r, mine, opposite_place, fresh(2, None, r, True))
        else:
            lax.fori_loop(0, opposite_place + 1, lambda j, _: back(2, None, r, mine, j, lambda keys, qs: lambda c: p_vm[j, c]), None)
        dq_out(2, None, r)

    def dkv_out(s):
        here = pl.ds(start_of(s), rows)
        dqkv_vm[s, :, width : width + d] = turn(dk_s[here, :] * scale, s, -1).astype(BF16)
        dqkv_vm[s, :, width + d :] = dv_s[here, :].astype(BF16)

    dkv_out(2)
    put(dy_vm.at[2], dy_out.at[2], 4).wait()

    def first(p):
        at = pl.ds(pl.multiple_of(p * eighth, eighth), eighth)
        return [send(dy_vm.at[2, low, at], in_vm.at[0, :, at], to_right, 30 + 2 * p), send(dy_vm.at[2, high, at], in_vm.at[1, :, at], to_left, 31 + 2 * p)]

    def count(t, s, at):
        unit = x_vm[s, :, at].astype(F32) * jnp.concatenate([scale_s[s]] * (t.shape[1] // 128), axis=1)
        both = t.astype(F32) * unit
        gain_s[:, at] += both.reshape(rows // 8, 8, t.shape[1]).sum(0)
        both = both * gain_vm[:, at]
        dots_vm[s] += sum(both[:, m : m + 128] for m in range(0, t.shape[1], 128))

    def opposite(c, _):
        at = pl.ds(pl.multiple_of(c * eighth, eighth), eighth)
        t = _dot(dqkv_vm[2], w_vm[at, :], 1, 1).astype(BF16)
        dy_vm[2, :, at] = t

        @pl.when(c < 7)
        def _():
            for k in first(c):
                k.start()

        count(t, 2, at)

    lax.fori_loop(0, 8, opposite, None)
    for s in (0, 1, n - 1):
        dkv_out(s)
        put(dy_vm.at[s], dy_out.at[s], 2 + s).wait()
    put(dqkv_vm, dqkv_out, 6).start()
    for c in x_ring + dy_ring + [c for r in range(2) for q in range(4) for c in far(r, q)]:
        c.wait_send()

    def others(c, _):
        at = pl.ds(pl.multiple_of(c * TILE, TILE), TILE)
        slots = (1, n - 1, 0)
        t = _dot(jnp.concatenate([dqkv_vm[s] for s in slots], axis=0), w_vm[at, :], 1, 1).astype(BF16)
        for m, s in enumerate(slots):
            dy_vm[s, :, at] = t[m * rows : (m + 1) * rows, :]
            count(t[m * rows : (m + 1) * rows, :], s, at)

    lax.fori_loop(0, deep // TILE, others, None)
    share = gain_s[...].sum(0, keepdims=True)
    for s in range(n):
        share_vm[s, :, :deep] = share
        share_vm[s, :, deep:] = dots_vm[s].T.sum(0, keepdims=True)
    shares_vm[me] = share_vm[0]
    shares = [send(share_vm.at[o], shares_vm.at[me], lax.rem(me + o, n), 45 + o) for o in range(1, n)]
    for c in shares + first(7):
        c.start()
    ends = [put(dy_vm.at[0], own_out, 7), put(dy_vm.at[1, high], right_b_out, 8), put(dy_vm.at[n - 1, low], left_a_out, 9), put(shares_vm, share_out, 10)]
    for c in ends[:3]:
        c.start()

    def sums(p):
        at = pl.ds(pl.multiple_of(p * eighth, eighth), eighth)
        return [put(in_vm.at[0, :, at], sum_a_out.at[:, at], 14 + 2 * p), put(in_vm.at[1, :, at], sum_b_out.at[:, at], 15 + 2 * p)]

    def add(p, _):
        at = pl.ds(pl.multiple_of(p * eighth, eighth), eighth)
        for c in first(p):
            c.wait_recv()
        in_vm[0, :, at] = (dy_vm[1, :half, at].astype(F32) + in_vm[0, :, at].astype(F32)).astype(BF16)
        in_vm[1, :, at] = (dy_vm[n - 1, half:, at].astype(F32) + in_vm[1, :, at].astype(F32)).astype(BF16)
        for c in sums(p):
            c.start()

    lax.fori_loop(0, 7, add, None)
    for c in shares:
        c.wait_recv()
    ends[3].start()
    add(7, None)
    for c in shares:
        c.wait_send()
    for p in range(8):
        for c in first(p):
            c.wait_send()
        ends += sums(p)
    for c in ends + [put(seen_vm, seen_out, 1), put(dqkv_vm, dqkv_out, 6)]:
        c.wait()


def gathered(n, x, dy, gain, wq, wk, wv, wo, table):
    rows, deep = x.shape
    width, d = wq.shape[1], wk.shape[1]
    g, half = width // d, rows // 2
    strips = g * rows // STRIP
    some = pl.BlockSpec(memory_space=pl.ANY)
    out = jax.ShapeDtypeStruct
    return pl.pallas_call(
        functools.partial(_kernel, n),
        in_specs=[some, some, pl.BlockSpec(memory_space=pltpu.VMEM)] + [some] * 5,
        out_specs=[some] * 10,
        out_shape=[out((n, 2, half, deep), BF16), out((n, rows, deep), BF16), out((n, rows, width), BF16), out((n, rows, width + 2 * d), BF16),
                   out((rows, deep), BF16)] + [out((half, deep), BF16)] * 4 + [out((n, 1, deep + rows), F32)],
        scratch_shapes=[
            pltpu.VMEM((n, rows, deep), BF16), pltpu.VMEM((deep, width + 2 * d), BF16),
            pltpu.VMEM((width, deep), BF16), pltpu.VMEM((n, rows, deep), BF16), pltpu.VMEM((n, rows, width), BF16),
            pltpu.VMEM((n, rows, width), BF16), pltpu.VMEM((rows, width), BF16), pltpu.VMEM((n, rows, width + 2 * d), BF16),
            pltpu.VMEM((n * rows, d), BF16), pltpu.VMEM((n * rows, d), BF16), pltpu.VMEM((n * rows, d), F32), pltpu.VMEM((n * rows, d), F32),
            pltpu.VMEM((n, strips, STRIP), F32), pltpu.VMEM((strips, STRIP), F32), pltpu.VMEM((strips, d + 8, STRIP), F32),
            pltpu.VMEM((strips, STRIP), F32), pltpu.VMEM((n * rows, d), F32), pltpu.VMEM((n * rows, d), F32),
            pltpu.VMEM((n, rows, 128), F32), pltpu.VMEM((2, half, deep), BF16), pltpu.VMEM((n, 1, deep + rows), F32), pltpu.VMEM((n, 1, deep + rows), F32),
            pltpu.VMEM((1, deep), F32), pltpu.VMEM((8, deep), F32), pltpu.VMEM((n, rows, 128), F32),
            pltpu.VMEM((n, strips // 2, rows, STRIP), F32), pltpu.VMEM((half, width), F32),
            pltpu.SemaphoreType.DMA((49,)), pltpu.SemaphoreType.DMA((49,)), pltpu.SemaphoreType.DMA((7,)), pltpu.SemaphoreType.DMA((30,)),
        ],
        compiler_params=pltpu.CompilerParams(collective_id=0, has_side_effects=True, vmem_limit_bytes=VMEM),
        cost_estimate=pl.CostEstimate(flops=60 * rows * deep * width, transcendentals=0, bytes_accessed=20 * rows * deep),
    )(x, dy, gain, wq, wk, wv, wo, table)


def _outer(a_ref, b_ref, *outs):
    t = _dot(a_ref[...], b_ref[...], 0, 0).astype(BF16)
    at = 0
    for o in outs:
        o[...] = t[:, at : at + o.shape[1]]
        at += o.shape[1]


def outer(a, b, widths):
    tokens, deep = a.shape
    tile = 2 * TILE
    return pl.pallas_call(
        _outer,
        grid=(deep // tile,),
        in_specs=[pl.BlockSpec((tokens, tile), lambda i: (0, i)), pl.BlockSpec(b.shape, lambda i: (0, 0))],
        out_specs=[pl.BlockSpec((tile, w), lambda i: (i, 0)) for w in widths],
        out_shape=[jax.ShapeDtypeStruct((deep, w), BF16) for w in widths],
        compiler_params=pltpu.CompilerParams(dimension_semantics=("arbitrary",), vmem_limit_bytes=24 * 2**20),
        cost_estimate=pl.CostEstimate(flops=2 * tokens * deep * b.shape[1], transcendentals=0, bytes_accessed=2 * deep * (tokens + b.shape[1])),
    )(a, b)


def solution(mesh):
    n = mesh.shape["tp"]

    def step(x, dy, gain, wq, wk, wv, wo):
        rows, deep = x.shape
        width = wq.shape[1]

        half_head = HEAD // 2
        rate = np.float32(THETA) ** (-np.arange(half_head, dtype=np.float32) / np.float32(half_head))
        angle = np.arange(n * rows, dtype=np.float32)[:, None] * rate
        table = jnp.asarray(np.concatenate([np.cos(angle), np.sin(angle)], 1))

        normal, dy_all, seen, dqkv, own, right_b, left_a, sum_a, sum_b, shares = gathered(n, x, dy, gain, wq, wk, wv, wo, table)

        def moved(t, places):
            return lax.ppermute(t, "tp", [(i, (i + places) % n) for i in range(n)])

        own_b, own_a = moved(right_b, 1), moved(left_a, -1)
        last_a, last_b = moved(sum_a, 1), moved(sum_b, -1)

        normal, dy_all, seen, dqkv = (t.reshape(n * rows, -1) for t in (normal, dy_all, seen, dqkv))
        by_wo = _dot(seen, dy_all, 0, 0).astype(BF16)
        by_wq, by_wk, by_wv = outer(normal, dqkv, (width, HEAD, HEAD))

        shares = shares.sum((0, 1))
        by_gain, mean = shares[None, :deep], shares[deep:, None] / deep

        wide, gain = x.astype(F32), gain.astype(F32)
        scale = lax.rsqrt(jnp.mean(wide * wide, -1, keepdims=True) + 1e-6)
        most = scale * ((own.astype(F32) + jnp.concatenate([own_a, own_b]).astype(F32)) * gain - wide * scale * mean) + dy.astype(F32)
        most = lax.optimization_barrier(most)
        by_x = most + scale * gain * jnp.concatenate([last_a, last_b]).astype(F32)
        return by_x.astype(BF16), by_gain, by_wq, by_wk, by_wv, by_wo

    tokens, columns = P(("dp", "tp"), None), P(None, "tp")
    return jax.shard_map(
        step,
        mesh=mesh,
        in_specs=(tokens, tokens, P(None), columns, columns, columns, P("tp", None)),
        out_specs=(tokens, P("dp", None), P("dp", "tp"), P("dp", "tp"), P("dp", "tp"), P(("dp", "tp"), None)),
        check_vma=False,
    )
```

```python
import functools

import jax
import jax.numpy as jnp
import numpy as np
from jax import lax
from jax.experimental import pallas as pl
from jax.experimental.pallas import tpu as pltpu
from jax.sharding import PartitionSpec as P

HEAD = 128
THETA = 10000
NEG = -1e30
HIDDEN = 2 * NEG
LOG2E = 1.4426950408889634
VMEM = 67043328
STRIP = 512
TILE = 256
F32, BF16 = jnp.float32, jnp.bfloat16


def _dot(a, b, ca, cb):
    return lax.dot_general(a, b, (((ca,), (cb,)), ((), ())), preferred_element_type=F32)


def _later(bk, cols, bq, first=0, jump=0):
    query = lax.rem(lax.broadcasted_iota(jnp.int32, (bk, cols), 1), bq)
    if jump:
        query += jnp.where(query >= bq // 2, jump, 0)
    return query + first >= lax.broadcasted_iota(jnp.int32, (bk, cols), 0)


def _kernel(n, x_ref, dy_ref, gain_ref, wq_ref, wk_ref, wv_ref, wo_ref, table_ref,
            a_out, dy_out, seen_out, dqkv_out, own_out, right_b_out, left_a_out, sum_a_out, sum_b_out, share_out,
            x_vm, w_vm, wo_vm, dy_vm, q_vm, seen_vm, ds_vm, dqkv_vm, k_vm, v_vm, dk_s, dv_s, lse_s, top_s, mix_s, delta_s,
            cos_vm, sin_vm, scale_s, in_vm, share_vm, shares_vm, gain_vm, gain_s, dots_vm, p_vm, acc_s, send_sem, recv_sem, load_sem, out_sem):
    rows, deep = x_ref.shape
    half = rows // 2
    d = k_vm.shape[1]
    dq_s, a_vm = mix_s.at[:, :d, :], in_vm
    width = wq_ref.shape[1]
    g = width // d
    per = STRIP // rows
    strips = g // per
    scale = d**-0.5
    e = scale * LOG2E
    me = lax.axis_index("tp")
    to_right, to_left = lax.rem(me + 1, n), lax.rem(me + n - 1, n)
    low, high = pl.ds(0, half), pl.ds(half, half)

    def start_of(s):
        return pl.multiple_of(lax.rem(me + s, n) * rows, rows)

    def send(src, dst, to, i):
        return pltpu.make_async_remote_copy(src_ref=src, dst_ref=dst, send_sem=send_sem.at[i], recv_sem=recv_sem.at[i],
                                            device_id={"tp": to}, device_id_type=pl.DeviceIdType.MESH)

    def load(src, dst, i):
        return pltpu.make_async_copy(src, dst, load_sem.at[i])

    def put(src, dst, i):
        return pltpu.make_async_copy(src, dst, out_sem.at[i])

    def ring(own, at, i):
        return [send(own.at[low], at.at[n - 1, low], to_right, i), send(own.at[high], at.at[1, high], to_left, i + 1),
                send(own.at[high], at.at[n - 1, high], to_right, i + 2), send(own.at[low], at.at[1, low], to_left, i + 3),
                send(at.at[n - 1, low], at.at[2, low], to_right, i + 4), send(at.at[1, high], at.at[2, high], to_left, i + 5)]

    quarter, eighth = deep // 4, deep // 8

    def far(r, q):
        at = pl.ds(pl.multiple_of(q * eighth, eighth), eighth)
        mine = [pl.ds(first + r * (half // 2), half // 2) for first in (0, half)]
        return [send(dy_vm.at[n - 1, mine[0], at], dy_vm.at[2, mine[0], at], to_right, 10 + 16 * r + 2 * q),
                send(dy_vm.at[1, mine[1], at], dy_vm.at[2, mine[1], at], to_left, 11 + 16 * r + 2 * q)]

    x_ring, dy_ring = ring(x_ref, x_vm, 0), ring(dy_ref, dy_vm, 6)[:4]
    loads = [load(x_ref, x_vm.at[0], 0), load(wq_ref, w_vm.at[:, pl.ds(0, width)], 1), load(wk_ref, w_vm.at[:, pl.ds(width, d)], 2),
             load(wv_ref, w_vm.at[:, pl.ds(width + d, d)], 3), load(table_ref, cos_vm, 4), load(dy_ref, dy_vm.at[0], 5), load(wo_ref, wo_vm, 6)]

    barrier = pltpu.get_barrier_semaphore()
    for neighbour in (to_right, to_left):
        pl.semaphore_signal(barrier, inc=1, device_id={"tp": neighbour}, device_id_type=pl.DeviceIdType.MESH)
    pl.semaphore_wait(barrier, 2)
    for c in x_ring[:4]:
        c.start()
    for c in loads:
        c.start()

    gain_vm[...] = gain_ref[...].astype(F32).reshape(1, deep)

    def turn(t, s, sign, at=0):
        here = pl.ds(pl.multiple_of(start_of(s) + at, half // 2), t.shape[0])
        return t * cos_vm[here, :] + sign * (pltpu.roll(t, d // 2, 1) * sin_vm[here, :])

    def project(i, _):
        s = i + i // 2 - 2 * (i // 3)

        @pl.when(i == 0)
        def _():
            for c in loads[:5]:
                c.wait()
            table = cos_vm[...]
            other = pltpu.roll(table, d // 2, 1)
            left_half = lax.broadcasted_iota(jnp.int32, table.shape, 1) < d // 2
            cos_vm[...] = jnp.where(left_half, table, other)
            sin_vm[...] = jnp.where(left_half, -other, table)

        @pl.when(i == 1)
        def _():
            for c in x_ring[:2]:
                c.wait_recv()
            for c in x_ring[4:] + dy_ring:
                c.start()
            for c in x_ring[2:4]:
                c.wait_recv()

        @pl.when(i == 3)
        def _():
            for c in x_ring[4:]:
                c.wait_recv()

        @pl.when(i > 0)
        def _():
            put(a_vm, a_out.at[0], 0).wait()

        def norm(r, _):
            some = pl.ds(pl.multiple_of(r * 16, 16), 16)
            t = x_vm[s, some, :].astype(F32)
            factor = lax.rsqrt(jnp.mean(t * t, -1, keepdims=True) + 1e-6)
            scale_s[s, some, :] = jnp.broadcast_to(factor, (16, 128))
            a_vm[r // (half // 16), pl.ds(pl.multiple_of(lax.rem(r * 16, half), 16), 16), :] = (t * factor * gain_vm[...]).astype(BF16)

        lax.fori_loop(0, rows // 16, norm, None)
        put(a_vm, a_out.at[s], 0).start()

        def tile(c, _):
            at = pl.multiple_of(c * TILE, TILE)
            t = _dot(a_vm[...].reshape(rows, deep), w_vm[:, pl.ds(at, TILE)], 1, 0).astype(BF16).astype(F32)
            for m in range(TILE // d):
                q_vm[s, :, pl.ds(pl.multiple_of(at + m * d, d), d)] = turn(t[:, m * d : (m + 1) * d], s, 1).astype(BF16)

        lax.fori_loop(0, width // TILE, tile, None)
        t = _dot(a_vm[...].reshape(rows, deep), w_vm[:, width:], 1, 0).astype(BF16)
        k_vm[pl.ds(start_of(s), rows), :] = turn(t[:, :d].astype(F32), s, 1).astype(BF16)
        v_vm[pl.ds(start_of(s), rows), :] = t[:, d:]

    lax.fori_loop(0, n, project, None)

    def heads(ref, first):
        return jnp.concatenate([ref[:, h * d : (h + 1) * d] for h in range(first, first + per)], axis=0)

    ones = jnp.ones((8, rows), BF16)

    def forward(s, _):
        top_s[...] = jnp.full_like(top_s, NEG)
        mix_s[...] = jnp.zeros_like(mix_s)

        def block(j, masked):
            here = pl.ds(pl.multiple_of(j * rows, rows), rows)
            keys = k_vm[here, :]
            values = jnp.concatenate([v_vm[here, :].T, ones], axis=0)
            scores = [_dot(keys, heads(q_vm.at[s], c * per), 1, 1) for c in range(strips)]
            weights, keeps = [], []
            for c, t in enumerate(scores):
                if masked:
                    t = jnp.where(_later(rows, STRIP, rows), t, HIDDEN)
                old = top_s[c : c + 1, :]
                top = jnp.maximum(old, t.max(axis=0, keepdims=True))
                top_s[c : c + 1, :] = top
                weights.append(jnp.exp2((t - top) * e).astype(BF16))
                keeps.append(jnp.exp2((old - top) * e))
            for c in range(strips):
                mix_s[c] = mix_s[c] * keeps[c] + _dot(values, weights[c], 1, 0)

        whole = lax.rem(me + s, n)
        lax.fori_loop(0, whole, lambda j, _: block(j, False), None)
        block(whole, True)
        for c in range(strips):
            total = mix_s[c, d : d + 1, :]
            out = (mix_s[c, :d, :] * (1 / total)).T
            lse_s[s, c : c + 1, :] = top_s[c : c + 1, :] * e + jnp.log(total) * LOG2E
            for m in range(per):
                h = c * per + m
                seen_vm[s, :, h * d : (h + 1) * d] = out[m * rows : (m + 1) * rows, :].astype(BF16)

    lax.fori_loop(0, n, forward, None)
    put(seen_vm, seen_out, 1).start()

    dk_s[...] = jnp.zeros_like(dk_s)
    dv_s[...] = jnp.zeros_like(dv_s)

    each = STRIP // half

    def pieces(at, r):
        return [pl.ds(at, half)] if at is not None else [pl.ds(first + r * (half // 2), half // 2) for first in (0, half)]

    def parts(ref, there):
        return [jnp.concatenate([ref[k, h * d : (h + 1) * d] for h in range(c, c + each) for k in there], axis=0) for c in range(0, g, each)]

    def delta(s, at, r, mine):
        for h in range(g):
            cols = slice(h * d, (h + 1) * d)
            seen = jnp.concatenate([seen_vm[s, k, cols] for k in pieces(at, r)], axis=0)
            both = ds_vm[mine, cols].astype(F32) * seen.astype(F32)
            c, m = divmod(h, each)
            delta_s[c : c + 1, m * half : (m + 1) * half] = both.T.sum(axis=0, keepdims=True)

    def lse_of(s, at, r, h):
        k, m = divmod(h, per)
        if at is not None:
            return lse_s[s, k : k + 1, pl.ds(pl.multiple_of(m * rows + at, half), half)]
        low, high = (lse_s[s, k : k + 1, m * rows + first : m * rows + first + half] for first in (0, half))
        first = lax.broadcasted_iota(jnp.int32, low.shape, 1) < half // 2
        return jnp.where(first, low, pltpu.roll(high, half // 2, 1)) if r == 0 else jnp.where(first, pltpu.roll(low, half // 2, 1), high)

    def weigh(s, at, r, c, scores, masked):
        p = jnp.exp2(scores * e - jnp.concatenate([lse_of(s, at, r, h) for h in range(c * each, (c + 1) * each)], axis=1))
        if not masked:
            return p
        return jnp.where(_later(rows, STRIP, half, at) if at is not None else _later(rows, STRIP, half, r * (half // 2), half // 2), p, 0.0)

    def fresh(s, at, r, masked):
        def weights(keys, qs):
            scores = [_dot(keys, t, 1, 1) for t in qs]
            return lambda c: weigh(s, at, r, c, scores[c], masked)
        return weights

    def back(s, at, r, mine, j, weights):
        here = pl.ds(pl.multiple_of(j * rows, rows), rows)
        keys, values = k_vm[here, :], v_vm[here, :]
        qs, dos = parts(q_vm.at[s], pieces(at, r)), parts(ds_vm, [mine])
        ps = weights(keys, qs)
        dps = [_dot(values, t, 1, 1) for t in dos]
        for c in range(len(qs)):
            p = ps(c)
            ds = (p * (dps[c] - delta_s[c : c + 1, :])).astype(BF16)
            dv_s[here, :] += _dot(p.astype(BF16), dos[c], 1, 0)
            dk_s[here, :] += _dot(ds, qs[c], 1, 0)
            dq_s[c] += _dot(keys.T, ds, 1, 0)

    def dq_out(s, at, r):
        for h in range(g):
            c, m = divmod(h, each)
            dq = (dq_s[c, :, m * half : (m + 1) * half] * scale).T
            some = pieces(at, r)
            long = half // len(some)
            for k, there in enumerate(some):
                dqkv_vm[s, there, h * d : (h + 1) * d] = turn(dq[k * long : (k + 1) * long, :], s, -1, there.start).astype(BF16)

    opposite_place = lax.rem(me + 2, n)

    def ahead(j, masked):
        keys = k_vm[pl.ds(pl.multiple_of(j * rows, rows), rows), :]
        for c, t in enumerate(parts(q_vm.at[2], pieces(None, 1))):
            p_vm[j, c] = weigh(2, None, 1, c, _dot(keys, t, 1, 1), masked)

    def near(i, _):
        pair, second = i // 2, lax.rem(i, 2)
        s = ((pair + 1) // 2) * (n - 1 - 2 * second)
        at = pl.multiple_of(half * lax.rem(second + pair // 2, 2), half)

        @pl.when(i == 0)
        def _():
            for c in loads[5:]:
                c.wait()
            put(dy_vm.at[0], dy_out.at[0], 2).start()

        @pl.when(i == 2)
        def _():
            put(a_vm, a_out.at[0], 0).wait()
            for c in dy_ring[:2]:
                c.wait_recv()
            for r in range(2):
                for q in range(8):
                    for c in far(r, q):
                        c.start()

        @pl.when(i == 4)
        def _():
            lax.fori_loop(0, opposite_place, lambda j, _: ahead(j, False), None)
            ahead(opposite_place, True)
            for c in dy_ring[2:]:
                c.wait_recv()
            for k in (1, n - 1):
                put(dy_vm.at[k], dy_out.at[k], 2 + k).start()

        @pl.when(second == 0)
        def _():
            other = (pair + 1) // 2
            there = pl.ds(pl.multiple_of(half - at, half), half)

            def tile(c, _):
                cols = pl.ds(pl.multiple_of(c * TILE, TILE), TILE)
                both = jnp.concatenate([dy_vm[s, pl.ds(at, half), :], dy_vm[other, there, :]], axis=0)
                ds_vm[:, cols] = _dot(both, wo_vm[cols, :], 1, 1).astype(BF16)

            lax.fori_loop(0, width // TILE, tile, None)

        mine = pl.ds(pl.multiple_of(second * half, half), half)
        dq_s[...] = jnp.zeros_like(dq_s)
        delta(s, at, None, mine)
        whole = lax.rem(me + s, n)
        lax.fori_loop(0, whole, lambda j, _: back(s, at, None, mine, j, fresh(s, at, None, False)), None)
        back(s, at, None, mine, whole, fresh(s, at, None, True))
        dq_out(s, at, None)

    lax.fori_loop(0, 6, near, None)

    gain_s[...] = jnp.zeros_like(gain_s)
    dots_vm[...] = jnp.zeros_like(dots_vm)
    for r in range(2):
        mine = pl.ds(r * half, half)
        dq_s[...] = jnp.zeros_like(dq_s)
        acc_s[...] = jnp.zeros_like(acc_s)

        def through(q, _):
            for c in far(r, q):
                c.wait_recv()
            part = pl.ds(pl.multiple_of(q * eighth, eighth), eighth)

            both = jnp.concatenate([dy_vm[2, k, part] for k in pieces(None, r)], axis=0)
            acc_s[...] += _dot(both, wo_vm[:, part], 1, 1)

        lax.fori_loop(0, 8, through, None)
        if r == 1:
            put(dy_vm.at[2], dy_out.at[2], 4).start()
        ds_vm[mine, :] = acc_s[...].astype(BF16)
        delta(2, None, r, mine)
        if r == 0:
            lax.fori_loop(0, opposite_place, lambda j, _: back(2, None, r, mine, j, fresh(2, None, r, False)), None)
            back(2, None, r, mine, opposite_place, fresh(2, None, r, True))
        else:
            lax.fori_loop(0, opposite_place + 1, lambda j, _: back(2, None, r, mine, j, lambda keys, qs: lambda c: p_vm[j, c]), None)
        dq_out(2, None, r)

    def dkv_out(s):
        here = pl.ds(start_of(s), rows)
        dqkv_vm[s, :, width : width + d] = turn(dk_s[here, :] * scale, s, -1).astype(BF16)
        dqkv_vm[s, :, width + d :] = dv_s[here, :].astype(BF16)

    dkv_out(2)
    put(dy_vm.at[2], dy_out.at[2], 4).wait()

    def first(p):
        at = pl.ds(pl.multiple_of(p * eighth, eighth), eighth)
        return [send(dy_vm.at[2, low, at], in_vm.at[0, :, at], to_right, 42 + 2 * p), send(dy_vm.at[2, high, at], in_vm.at[1, :, at], to_left, 43 + 2 * p)]

    def count(t, s, at):
        unit = x_vm[s, :, at].astype(F32) * jnp.concatenate([scale_s[s]] * (t.shape[1] // 128), axis=1)
        both = t.astype(F32) * unit
        gain_s[:, at] += both.reshape(rows // 8, 8, t.shape[1]).sum(0)
        both = both * gain_vm[:, at]
        dots_vm[s] += sum(both[:, m : m + 128] for m in range(0, t.shape[1], 128))

    def opposite(c, _):
        at = pl.ds(pl.multiple_of(c * eighth, eighth), eighth)
        t = _dot(dqkv_vm[2], w_vm[at, :], 1, 1).astype(BF16)
        dy_vm[2, :, at] = t

        @pl.when(c < 7)
        def _():
            for k in first(c):
                k.start()

        count(t, 2, at)

    lax.fori_loop(0, 8, opposite, None)
    for s in (0, 1, n - 1):
        dkv_out(s)
        put(dy_vm.at[s], dy_out.at[s], 2 + s).wait()
    put(dqkv_vm, dqkv_out, 6).start()
    for c in x_ring + dy_ring + [c for r in range(2) for q in range(8) for c in far(r, q)]:
        c.wait_send()

    def others(c, _):
        at = pl.ds(pl.multiple_of(c * TILE, TILE), TILE)
        slots = (1, n - 1, 0)
        t = _dot(jnp.concatenate([dqkv_vm[s] for s in slots], axis=0), w_vm[at, :], 1, 1).astype(BF16)
        for m, s in enumerate(slots):
            dy_vm[s, :, at] = t[m * rows : (m + 1) * rows, :]
            count(t[m * rows : (m + 1) * rows, :], s, at)

    lax.fori_loop(0, deep // TILE, others, None)
    share = gain_s[...].sum(0, keepdims=True)
    for s in range(n):
        share_vm[s, :, :deep] = share
        share_vm[s, :, deep:] = dots_vm[s].T.sum(0, keepdims=True)
    shares_vm[me] = share_vm[0]
    shares = [send(share_vm.at[o], shares_vm.at[me], lax.rem(me + o, n), 57 + o) for o in range(1, n)]
    for c in shares + first(7):
        c.start()
    ends = [put(dy_vm.at[0], own_out, 7), put(dy_vm.at[1, high], right_b_out, 8), put(dy_vm.at[n - 1, low], left_a_out, 9), put(shares_vm, share_out, 10)]
    for c in ends[:3]:
        c.start()

    def sums(p):
        at = pl.ds(pl.multiple_of(p * eighth, eighth), eighth)
        return [put(in_vm.at[0, :, at], sum_a_out.at[:, at], 14 + 2 * p), put(in_vm.at[1, :, at], sum_b_out.at[:, at], 15 + 2 * p)]

    def add(p, _):
        at = pl.ds(pl.multiple_of(p * eighth, eighth), eighth)
        for c in first(p):
            c.wait_recv()
        in_vm[0, :, at] = (dy_vm[1, :half, at].astype(F32) + in_vm[0, :, at].astype(F32)).astype(BF16)
        in_vm[1, :, at] = (dy_vm[n - 1, half:, at].astype(F32) + in_vm[1, :, at].astype(F32)).astype(BF16)
        for c in sums(p):
            c.start()

    lax.fori_loop(0, 7, add, None)
    for c in shares:
        c.wait_recv()
    ends[3].start()
    add(7, None)
    for c in shares:
        c.wait_send()
    for p in range(8):
        for c in first(p):
            c.wait_send()
        ends += sums(p)
    for c in ends + [put(seen_vm, seen_out, 1), put(dqkv_vm, dqkv_out, 6)]:
        c.wait()


def gathered(n, x, dy, gain, wq, wk, wv, wo, table):
    rows, deep = x.shape
    width, d = wq.shape[1], wk.shape[1]
    g, half = width // d, rows // 2
    strips = g * rows // STRIP
    some = pl.BlockSpec(memory_space=pl.ANY)
    out = jax.ShapeDtypeStruct
    return pl.pallas_call(
        functools.partial(_kernel, n),
        in_specs=[some, some, pl.BlockSpec(memory_space=pltpu.VMEM)] + [some] * 5,
        out_specs=[some] * 10,
        out_shape=[out((n, 2, half, deep), BF16), out((n, rows, deep), BF16), out((n, rows, width), BF16), out((n, rows, width + 2 * d), BF16),
                   out((rows, deep), BF16)] + [out((half, deep), BF16)] * 4 + [out((n, 1, deep + rows), F32)],
        scratch_shapes=[
            pltpu.VMEM((n, rows, deep), BF16), pltpu.VMEM((deep, width + 2 * d), BF16),
            pltpu.VMEM((width, deep), BF16), pltpu.VMEM((n, rows, deep), BF16), pltpu.VMEM((n, rows, width), BF16),
            pltpu.VMEM((n, rows, width), BF16), pltpu.VMEM((rows, width), BF16), pltpu.VMEM((n, rows, width + 2 * d), BF16),
            pltpu.VMEM((n * rows, d), BF16), pltpu.VMEM((n * rows, d), BF16), pltpu.VMEM((n * rows, d), F32), pltpu.VMEM((n * rows, d), F32),
            pltpu.VMEM((n, strips, STRIP), F32), pltpu.VMEM((strips, STRIP), F32), pltpu.VMEM((strips, d + 8, STRIP), F32),
            pltpu.VMEM((strips, STRIP), F32), pltpu.VMEM((n * rows, d), F32), pltpu.VMEM((n * rows, d), F32),
            pltpu.VMEM((n, rows, 128), F32), pltpu.VMEM((2, half, deep), BF16), pltpu.VMEM((n, 1, deep + rows), F32), pltpu.VMEM((n, 1, deep + rows), F32),
            pltpu.VMEM((1, deep), F32), pltpu.VMEM((8, deep), F32), pltpu.VMEM((n, rows, 128), F32),
            pltpu.VMEM((n, strips // 2, rows, STRIP), F32), pltpu.VMEM((half, width), F32),
            pltpu.SemaphoreType.DMA((61,)), pltpu.SemaphoreType.DMA((61,)), pltpu.SemaphoreType.DMA((7,)), pltpu.SemaphoreType.DMA((30,)),
        ],
        compiler_params=pltpu.CompilerParams(collective_id=0, has_side_effects=True, vmem_limit_bytes=VMEM),
        cost_estimate=pl.CostEstimate(flops=60 * rows * deep * width, transcendentals=0, bytes_accessed=20 * rows * deep),
    )(x, dy, gain, wq, wk, wv, wo, table)


def _outer(a_ref, b_ref, *outs):
    t = _dot(a_ref[...], b_ref[...], 0, 0).astype(BF16)
    at = 0
    for o in outs:
        o[...] = t[:, at : at + o.shape[1]]
        at += o.shape[1]


def outer(a, b, widths):
    tokens, deep = a.shape
    tile = 2 * TILE
    return pl.pallas_call(
        _outer,
        grid=(deep // tile,),
        in_specs=[pl.BlockSpec((tokens, tile), lambda i: (0, i)), pl.BlockSpec(b.shape, lambda i: (0, 0))],
        out_specs=[pl.BlockSpec((tile, w), lambda i: (i, 0)) for w in widths],
        out_shape=[jax.ShapeDtypeStruct((deep, w), BF16) for w in widths],
        compiler_params=pltpu.CompilerParams(dimension_semantics=("arbitrary",), vmem_limit_bytes=24 * 2**20),
        cost_estimate=pl.CostEstimate(flops=2 * tokens * deep * b.shape[1], transcendentals=0, bytes_accessed=2 * deep * (tokens + b.shape[1])),
    )(a, b)


def solution(mesh):
    n = mesh.shape["tp"]

    def step(x, dy, gain, wq, wk, wv, wo):
        rows, deep = x.shape
        width = wq.shape[1]

        half_head = HEAD // 2
        rate = np.float32(THETA) ** (-np.arange(half_head, dtype=np.float32) / np.float32(half_head))
        angle = np.arange(n * rows, dtype=np.float32)[:, None] * rate
        table = jnp.asarray(np.concatenate([np.cos(angle), np.sin(angle)], 1))

        normal, dy_all, seen, dqkv, own, right_b, left_a, sum_a, sum_b, shares = gathered(n, x, dy, gain, wq, wk, wv, wo, table)

        def moved(t, places):
            return lax.ppermute(t, "tp", [(i, (i + places) % n) for i in range(n)])

        own_b, own_a = moved(right_b, 1), moved(left_a, -1)
        last_a, last_b = moved(sum_a, 1), moved(sum_b, -1)

        normal, dy_all, seen, dqkv = (t.reshape(n * rows, -1) for t in (normal, dy_all, seen, dqkv))
        by_wo = _dot(seen, dy_all, 0, 0).astype(BF16)
        by_wq, by_wk, by_wv = outer(normal, dqkv, (width, HEAD, HEAD))

        shares = shares.sum((0, 1))
        by_gain, mean = shares[None, :deep], shares[deep:, None] / deep

        wide, gain = x.astype(F32), gain.astype(F32)
        scale = lax.rsqrt(jnp.mean(wide * wide, -1, keepdims=True) + 1e-6)
        most = scale * ((own.astype(F32) + jnp.concatenate([own_a, own_b]).astype(F32)) * gain - wide * scale * mean) + dy.astype(F32)
        most = lax.optimization_barrier(most)
        by_x = most + scale * gain * jnp.concatenate([last_a, last_b]).astype(F32)
        return by_x.astype(BF16), by_gain, by_wq, by_wk, by_wv, by_wo

    tokens, columns = P(("dp", "tp"), None), P(None, "tp")
    return jax.shard_map(
        step,
        mesh=mesh,
        in_specs=(tokens, tokens, P(None), columns, columns, columns, P("tp", None)),
        out_specs=(tokens, P("dp", None), P("dp", "tp"), P("dp", "tp"), P("dp", "tp"), P(("dp", "tp"), None)),
        check_vma=False,
    )
```
